512 devices in a mesh: dp: 32 (over z_lo, y, core), expert: 16 (over x, z_hi).
Axes of the slice: x: 4, y: 8, z: 8 (z_hi: 4, z_lo: 2; z = z_hi * 2 + z_lo), core: 2. Of those that a mesh axis runs over, the one named last changes fastest.
Arguments:
- grad_out: bfloat16 [4, 32768, 1024], P(None, ('dp', 'expert')), may hold values from -12 to 12
- routes: int32 [4, 32768, 8], P(None, ('dp', 'expert')), may hold values from 0 to 127, all different within a row; in each aligned block of 64 rows (0 to 63, 64 to 127, ..., all dimensions but the last counted through in order) at most 8 rows name the same one
- route_probs: bfloat16 [4, 32768, 8], P(None, ('dp', 'expert')), may hold values from 0.049804688 to 0.3984375
- dispatched: bfloat16 [4, 65536, 1024], P(None, ('dp', 'expert')), may hold values from -12 to 12, as said below
- w_gate: bfloat16 [1024, 4096], P(None, 'expert'), may hold values from -0.1875 to 0.1875
- w_up: bfloat16 [1024, 4096], P(None, 'expert'), may hold values from -0.1875 to 0.1875
- w_down: bfloat16 [4096, 1024], P('expert'), may hold values from -0.25 to 0.25
Outputs:
- grad_in: bfloat16 [4, 32768, 1024], P(None, ('dp', 'expert'))
- grad_gate: float32 [1024, 4096], P('dp', 'expert')
- grad_up: float32 [1024, 4096], P('dp', 'expert')
- grad_down_t: float32 [1024, 4096], P('dp', 'expert')
The draws below stay inside these ranges and needn't reach their ends.
Inputs may be any that keep to these rules, and one draw needn't show every extreme that they name: `routes`: in each micro-batch, among the 64 rows of one device no expert is named more than 8 times, a bound that some expert reaches in some of these blocks. `dispatched`: within each group of 16 consecutive blocks of 128 rows, blocks 2e and 2e + 1 are equal.
All inputs are finite; a program needn't handle non-finite values.
Results may differ from the reference program's by a relative error of at most 0.0058.
Values may be sent and summed in bfloat16 or wider, within the bound.
A program may use at most 64 MiB of HBM per device.

```python
import math
import jax
import jax.numpy as jnp
import numpy as np
from jax import lax

D = 1024
F = 512
NEXP = 128
TOPK = 8
MB = 4
TOK_DEV = 64
CAPS = 8
EXPERTS = 8
TOKENS = 32768
N_DP = 32
N_EXPERT = 16


def draw_dispatched(key, part):
    shape = (MB, N_DP, N_EXPERT // 2, N_EXPERT * CAPS, D)
    values = jax.random.truncated_normal(key, -4.0, 4.0, shape, jnp.float32)
    doubled = jnp.repeat(values, 2, axis=2)
    return doubled.reshape(MB, N_DP * N_EXPERT * N_EXPERT * CAPS, D).astype(jnp.bfloat16)


def levels(key, shape, shards, smallest, largest):
    gain, own = 1.0, jax.random.fold_in(key, 6)
    for dim, blocks in shards:
        steps = jnp.exp(jax.random.uniform(jax.random.fold_in(own, dim), (blocks,), jnp.float32, smallest / len(shards), largest / len(shards)))
        gain = gain * jnp.repeat(steps, shape[dim] // blocks).reshape([-1 if axis == dim else 1 for axis in range(len(shape))])
    return gain


def shared_out(rng, own, number, rows, number_of, top, limit, skew):
    sequence = jax.random.permutation(rng, number_of)
    heavy_load, ordinary = portions_of(number_of, rows * top, limit, skew, True), portions_of(number_of, rows * top, limit, skew, False)
    places = jnp.arange(number_of)

    def named(lengths, rotation):
        used = int((lengths > 0).sum())
        fixed = max(1, used // 4)
        passed = fixed + (places - fixed + rotation * (used - fixed)) % max(1, number_of - fixed)
        return jnp.zeros((number_of,), jnp.int32).at[sequence[jnp.where(places < fixed, places, passed)]].set(jnp.asarray(lengths, jnp.int32))

    lengths = jnp.where(number % 4 == 0, named(heavy_load, number // 4), named(ordinary, number - number // 4 - 1))
    mixed = jax.random.permutation(jax.random.fold_in(own, 3), number_of)
    source_of, taker = mixed[0:number_of // 2 * 2:2], mixed[1:number_of // 2 * 2:2]
    margin = jnp.minimum(lengths[source_of] - 1, limit - lengths[taker]) // 2
    margin = jnp.where((source_of == sequence[0]) | (taker == sequence[0]) | (lengths[taker] == 0), 0, jnp.maximum(margin, 0))
    passed = jax.random.randint(jax.random.fold_in(own, 4), (number_of // 2,), 0, 1 << 20) % (margin + 1)
    lengths = lengths.at[source_of].add(-passed).at[taker].add(passed)
    items = jnp.searchsorted(jnp.cumsum(lengths), jnp.arange(rows * top), side="right").astype(jnp.int32)
    table = items.reshape(top, rows).T
    table = table[jax.random.permutation(jax.random.fold_in(own, 1), rows)]
    rotation = jax.random.randint(jax.random.fold_in(own, 2), (rows, 1), 0, top)
    return jnp.take_along_axis(table, (jnp.arange(top)[None, :] + rotation) % top, axis=1)


def portions_of(count, total, reach, lean, full):
    loads = [(1 << 20) // math.isqrt(grade ** lean) + 1 for grade in range(1, count + 1)]
    largest = reach if full else min(reach, max(-(-total // count), total * loads[0] // sum(loads)))
    least = 1 if total - largest >= count - 1 else 0
    given, spare = [largest] + [least] * (count - 1), total - largest - least * (count - 1)
    while spare > 0:
        free = [i for i in range(1, count) if given[i] < largest] or [i for i in range(1, count) if given[i] < reach]
        pool, left = sum([loads[i] for i in free]), spare
        for i in free:
            addition = min(reach - given[i], max(1, left * loads[i] // pool), spare)
            given[i] = given[i] + addition
            spare = spare - addition
    return np.array(given)


def scatter_about(own_key, extent, deviation, bound, cuts=(), kind=jnp.bfloat16):
    result = jax.random.normal(own_key, extent, jnp.float32) * deviation
    if len(cuts) > 0:
        result = levels(own_key, extent, cuts, -0.22, 0.18) * result
    return jnp.clip(result, min=-bound, max=bound).astype(kind)


def setup_inputs(seed: int = 0) -> dict:
    splits = jax.random.split(jax.random.key(seed), 8)
    grad_out = scatter_about(splits[0], (MB, TOKENS, D), 3.0, 12.0, ((1, 512),))
    routes_keys = jax.random.split(jax.random.fold_in(splits[1], 1), MB * TOKENS // TOK_DEV)
    routes_turns = jax.random.permutation(jax.random.fold_in(splits[1], 3), MB * TOKENS // TOK_DEV)
    routes = jax.vmap(lambda own, number: shared_out(jax.random.fold_in(splits[1], 2), own, number, TOK_DEV, NEXP, TOPK, CAPS, 1))(routes_keys, routes_turns).reshape((MB, TOKENS, TOPK))
    route_probs = jnp.clip(0.049804688 + 0.3486328 * jax.random.uniform(splits[2], (MB, TOKENS, TOPK), jnp.float32) ** levels(splits[2], (MB, TOKENS, TOPK), ((1, 512),), -0.2, 0.2), 0.049804688, 0.3984375).astype(jnp.bfloat16)
    dispatched = draw_dispatched(jax.random.fold_in(splits[7], 71), 0)
    w_gate = scatter_about(splits[4], (D, EXPERTS * F), D ** -0.5, 0.1875, ((1, 16),))
    w_up = scatter_about(splits[5], (D, EXPERTS * F), D ** -0.5, 0.1875, ((1, 16),))
    w_down = scatter_about(splits[6], (EXPERTS * F, D), F ** -0.5, 0.25, ((0, 16),))
    return {"grad_out": grad_out, "routes": routes, "route_probs": route_probs, "dispatched": dispatched, "w_gate": w_gate, "w_up": w_up, "w_down": w_down}


def expert_backward(rows_in, row_grads, gate_mat, up_mat, down_mat):
    gate_pre = jnp.dot(rows_in, gate_mat, preferred_element_type=jnp.float32)
    up_pre = jnp.dot(rows_in, up_mat, preferred_element_type=jnp.float32)
    sigmoid = jax.nn.sigmoid(gate_pre)
    activated = gate_pre * sigmoid
    hidden = (activated * up_pre).astype(jnp.bfloat16)
    d_down = jnp.dot(row_grads.T, hidden, preferred_element_type=jnp.float32)
    dhidden = jnp.dot(row_grads, down_mat.T, preferred_element_type=jnp.float32)
    d_gate = (dhidden * up_pre * sigmoid * (1.0 + gate_pre * (1.0 - sigmoid))).astype(jnp.bfloat16)
    d_up = (dhidden * activated).astype(jnp.bfloat16)
    grad_gate_e = jnp.dot(rows_in.T, d_gate, preferred_element_type=jnp.float32)
    grad_up_e = jnp.dot(rows_in.T, d_up, preferred_element_type=jnp.float32)
    slot_grad = jnp.dot(d_gate, gate_mat.T, preferred_element_type=jnp.float32) + jnp.dot(d_up, up_mat.T, preferred_element_type=jnp.float32)
    return slot_grad, grad_gate_e, grad_up_e, d_down


def reference(grad_out, routes, route_probs, dispatched, w_gate, w_up, w_down):
    groups = N_EXPERT
    window = N_EXPERT // 2
    row_count = N_EXPERT * CAPS
    gate_blocks = w_gate.reshape(D, window, F).transpose(1, 0, 2)
    up_blocks = w_up.reshape(D, window, F).transpose(1, 0, 2)
    down_blocks = w_down.reshape(window, F, D)
    inputs = dispatched.reshape(MB * N_DP, groups, row_count, D)[:, ::2]
    out_grads = grad_out.reshape(MB * N_DP, groups * TOK_DEV, D)
    route_ids = routes.reshape(MB * N_DP, groups, TOK_DEV * TOPK)
    weights_all = route_probs.reshape(MB * N_DP, groups, TOK_DEV, TOPK)

    def group_step(totals, pieces):
        group_x, group_dy, group_ids, group_probs = pieces
        hitting = (group_ids[:, :, None] == jnp.arange(window, dtype=jnp.int32)[None, None, :]).astype(jnp.int32)
        ranking = jnp.sum((jnp.cumsum(hitting, axis=1) - 1) * hitting, axis=2)
        source = jnp.arange(groups, dtype=jnp.int32)[:, None]
        where_to = jnp.where(group_ids < window, group_ids * row_count + source * CAPS + ranking, window * row_count).astype(jnp.int32)
        scaled = (group_probs[..., None].astype(jnp.float32) * group_dy.reshape(groups, TOK_DEV, 1, D).astype(jnp.float32)).astype(jnp.bfloat16)
        buffer = jnp.zeros((window * row_count + 1, D), jnp.bfloat16).at[where_to.reshape(-1)].set(scaled.reshape(-1, D))
        slot_grads = buffer[:-1].reshape(window, row_count, D)

        def one_expert(packed):
            return expert_backward(packed[0], packed[1], packed[2], packed[3], packed[4])

        slot_grad, grad_gate_e, grad_up_e, d_down = lax.map(one_expert, (group_x, slot_grads, gate_blocks, up_blocks, down_blocks))
        padded = jnp.concatenate([slot_grad.reshape(window * row_count, D), jnp.zeros((1, D), jnp.float32)], axis=0)
        per_route = padded[where_to.reshape(-1)].reshape(groups * TOK_DEV, TOPK, D)
        grad_tokens = jnp.sum(per_route, axis=1).astype(jnp.bfloat16)
        totals = (totals[0] + grad_gate_e, totals[1] + grad_up_e, totals[2] + d_down)
        return totals, grad_tokens

    start = (jnp.zeros((window, D, F), jnp.float32), jnp.zeros((window, D, F), jnp.float32), jnp.zeros((window, D, F), jnp.float32))
    totals, grad_tokens = lax.scan(group_step, start, (inputs, out_grads, route_ids, weights_all))
    factor = 1.0 / (MB * N_DP)
    grad_gate = (totals[0] * factor).transpose(1, 0, 2).reshape(D, window * F)
    grad_up = (totals[1] * factor).transpose(1, 0, 2).reshape(D, window * F)
    grad_down_t = (totals[2] * factor).transpose(1, 0, 2).reshape(D, window * F)
    grad_in = grad_tokens.reshape(MB, N_DP * groups * TOK_DEV, D)
    return grad_in, grad_gate, grad_up, grad_down_t
```

```python
import jax
import jax.numpy as jnp
from jax import lax
from jax.experimental import pallas as pl
from jax.experimental.pallas import tpu as pltpu
from jax.sharding import PartitionSpec as P

MESH = pl.DeviceIdType.MESH
F32 = jnp.float32
BF16 = jnp.bfloat16

NT = (((1,), (1,)), ((), ()))
TN = (((0,), (0,)), ((), ()))


def kernel(
    dy_hbm, routes_hbm, probs_hbm, disp_hbm, wg_hbm, wu_hbm, wd_hbm,
    gin_ref, gg_ref, gu_ref, gd_ref,
    routes_v, probs_v, dy_v, x_v, wgu, wd, pgu, pd,
    mix_v, s_send, s_recv, act_v, fac_v, hid_v, dg_v, dgp_v, sg_v, ret_v,
    rf, rb, drecv, lsend, lrecv, ssend, srecv, fin, finb, z1, zd,
    in_sem, x_sem, self_sem, ret_self_sem,
    ds_sem, dr_sem, rs_sem, rr_sem,
    ws_sem, wr_sem, sws_sem, swr_sem, cs_sem, cr_sem,
    lss_sem, lsr_sem, sss_sem, ssr_sem, zs_sem, zr_sem,
):
    dp = lax.axis_index("dp")
    mem = lax.axis_index("expert")
    core = dp % 2
    y = (dp // 2) % 8
    zl = dp // 16
    step = 1 - 2 * core
    mine = mem // 2
    zh = mem % 4
    low = (zh * (3 - zh)) // 2

    def peer_of(e):
        return 4 * (e // 2) + low + (e % 2) * (3 - 2 * low)

    partner = mem + 1 - 2 * (mem % 2)
    dp_core = dp + 1 - 2 * core
    dp_fwd = zl * 16 + ((y + step + 8) % 8) * 2 + core
    dp_bwd = zl * 16 + ((y - step + 8) % 8) * 2 + core
    dp_z = (1 - zl) * 16 + y * 2 + core

    def remote(src, dst, ssem, rsem, dev):
        return pltpu.make_async_remote_copy(
            src_ref=src, dst_ref=dst, send_sem=ssem, recv_sem=rsem,
            device_id=dev, device_id_type=MESH,
        )

    barrier = pltpu.get_barrier_semaphore()
    peers = [(dp, peer_of((mine + i) % 8)) for i in range(1, 8)]
    peers += [(dp, partner), (dp_core, mem), (dp_fwd, mem), (dp_bwd, mem), (dp_z, mem), (dp_z, partner)]
    for dev in peers:
        pl.semaphore_signal(barrier, inc=1, device_id=dev, device_id_type=MESH)

    loads = [
        pltpu.make_async_copy(routes_hbm, routes_v, in_sem.at[0]),
        pltpu.make_async_copy(probs_hbm, probs_v, in_sem.at[1]),
        pltpu.make_async_copy(dy_hbm, dy_v, in_sem.at[2]),
        pltpu.make_async_copy(wg_hbm, wgu.at[:, :, :, :, pl.ds(0, 256)], in_sem.at[3]),
        pltpu.make_async_copy(wu_hbm, wgu.at[:, :, :, :, pl.ds(256, 256)], in_sem.at[4]),
        pltpu.make_async_copy(wd_hbm, wd, in_sem.at[5]),
    ]
    for load in loads:
        load.start()
    x_loads = []
    for side in range(2):
        lo = low if side == 0 else 1 - low
        for j in range(8):
            src = 4 * (j // 2) + (lo if j % 2 == 0 else 3 - lo)
            x_loads.append(
                pltpu.make_async_copy(
                    disp_hbm.at[:, pl.ds(pl.multiple_of(src * 8, 8), 8)],
                    x_v.at[side, :, pl.ds(j * 8, 8)],
                    x_sem.at[side, j],
                )
            )
    for load in x_loads:
        load.start()

    for load in loads[:3]:
        load.wait()

    def route(mb, carry):
        ids = routes_v[mb]
        probs = probs_v[mb].astype(F32)
        lane = lax.broadcasted_iota(jnp.int32, (64, 64), 1)
        row = lax.broadcasted_iota(jnp.int32, (64, 64), 0)
        expert = lax.shift_right_logical(lane, 3)
        place = lax.bitwise_and(lane, 7)
        hit = jnp.zeros((64, 64), F32)
        weight = jnp.zeros((64, 64), F32)
        for k in range(8):
            same = ids[:, k : k + 1] == expert
            hit = hit + jnp.where(same, 1.0, 0.0)
            weight = weight + jnp.where(same, probs[:, k : k + 1], 0.0)
        earlier = jnp.where(lane < row, 1.0, 0.0).astype(BF16)
        rank = jnp.dot(earlier, hit.astype(BF16), preferred_element_type=F32)
        chosen = jnp.where(rank == place.astype(F32), hit, 0.0)
        mix_v[mb] = chosen.astype(BF16)
        weighted = (chosen * weight).astype(BF16)
        scaled = lax.dot_general(weighted, dy_v[mb], TN, preferred_element_type=F32)
        s_send[mb] = scaled.astype(BF16)
        return carry

    lax.fori_loop(0, 4, route, 0)
    for load in loads[3:]:
        load.wait()
    pl.semaphore_wait(barrier, len(peers))

    sends = []
    quarter = y % 4

    def weights_copy(n, src_a, src_b, where, side, dev):
        copies = [
            remote(src_a.at[:, where, side], pgu.at[:, where, side], ws_sem.at[n, 0], wr_sem.at[n, 0], dev),
            remote(src_b.at[:, where, side], pd.at[:, where, side], ws_sem.at[n, 1], wr_sem.at[n, 1], dev),
        ]
        return copies

    def start(copies):
        for copy in copies:
            copy.start()
        sends.extend(copies)

    def weights_wait(n, where, side):
        for copy in weights_copy(n, pgu, pd, where, side, (dp_core, mem)):
            copy.wait_recv()

    start(weights_copy(0, wgu, wd, quarter, core, (dp, partner)))

    def slots_copy(src, dst, sem_s, sem_r, chunk, i):
        to = (mine + i) % 8
        return remote(
            src.at[pl.ds(2 * chunk, 2), pl.ds(pl.multiple_of(to * 8, 8), 8)],
            dst.at[pl.ds(2 * chunk, 2), pl.ds(pl.multiple_of(mine * 8, 8), 8)],
            sem_s.at[chunk, i - 1],
            sem_r.at[chunk, i - 1],
            (dp, peer_of(to)),
        )

    def slots_wait(src, dst, sem_s, sem_r, chunk, i):
        came = (mine + 8 - i) % 8
        remote(
            src.at[pl.ds(2 * chunk, 2), pl.ds(pl.multiple_of(came * 8, 8), 8)],
            dst.at[pl.ds(2 * chunk, 2), pl.ds(pl.multiple_of(came * 8, 8), 8)],
            sem_s.at[chunk, i - 1],
            sem_r.at[chunk, i - 1],
            (dp, peer_of((mine + i) % 8)),
        ).wait_recv()

    def slots_self(src, dst, sem, chunk):
        at = pl.ds(pl.multiple_of(mine * 8, 8), 8)
        return pltpu.make_async_copy(
            src.at[pl.ds(2 * chunk, 2), at], dst.at[pl.ds(2 * chunk, 2), at], sem.at[chunk]
        )

    for chunk in range(2):
        start([slots_copy(s_send, s_recv, ds_sem, dr_sem, chunk, i) for i in range(1, 8)])
    for chunk in range(2):
        slots_self(s_send, s_recv, self_sem, chunk).start()

    for load in x_loads:
        load.wait()

    def hidden(half, weights):
        def body(chunk, carry):
            rows = x_v[0, pl.ds(2 * chunk, 2)].reshape(128, 1024)
            both = jnp.dot(rows, weights[...].reshape(1024, 512), preferred_element_type=F32)
            gate, up = both[:, :256], both[:, 256:]
            sig = jax.nn.sigmoid(gate)
            act = gate * sig
            act_v[half, chunk] = act
            fac_v[half, chunk] = up * sig * (1.0 + gate * (1.0 - sig))
            hid_v[chunk, :, pl.ds(256 * half, 256)] = (act * up).astype(BF16)
            return carry

        lax.fori_loop(0, 2, body, 0)

    weights_wait(0, quarter, core)
    start(weights_copy(1, pgu, pd, quarter, core, (dp_fwd, mem)))
    start(weights_copy(2, pgu, pd, quarter, core, (dp_bwd, mem)))
    start(weights_copy(4, pgu, pd, quarter, core, (dp_core, mem)))
    hidden(0, wgu)
    from_bwd = (y - step + 8) % 4
    from_fwd = (y + step + 8) % 4
    across = (y + 2) % 4
    weights_wait(1, from_bwd, core)
    start(weights_copy(3, pgu, pd, from_bwd, core, (dp_fwd, mem)))
    start(weights_copy(5, pgu, pd, from_bwd, core, (dp_core, mem)))
    weights_wait(2, from_fwd, core)
    start(weights_copy(6, pgu, pd, from_fwd, core, (dp_core, mem)))
    weights_wait(3, across, core)
    start(weights_copy(7, pgu, pd, across, core, (dp_core, mem)))
    weights_wait(4, quarter, 1 - core)
    weights_wait(5, from_fwd, 1 - core)
    weights_wait(6, from_bwd, 1 - core)
    weights_wait(7, across, 1 - core)
    hidden(1, pgu)

    def slot_grads(chunk):
        rows = s_recv[pl.ds(2 * chunk, 2)].reshape(128, 1024)
        total = None
        for half, (down, both) in enumerate(((wd, wgu), (pd, pgu))):
            dh = lax.dot_general(rows, down[...].reshape(256, 1024), NT, preferred_element_type=F32)
            d_both = jnp.concatenate(
                [(dh * fac_v[half, chunk]).astype(BF16), (dh * act_v[half, chunk]).astype(BF16)], axis=1
            )
            if half == 0:
                dg_v[0, chunk] = d_both
            else:
                dgp_v[chunk] = d_both
            part = lax.dot_general(d_both, both[...].reshape(1024, 512), NT, preferred_element_type=F32)
            total = part if total is None else total + part
        sg_v[pl.ds(2 * chunk, 2)] = total.astype(BF16).reshape(2, 64, 1024)

    def swap_copy(chunk):
        return remote(
            dgp_v.at[chunk], dg_v.at[1, chunk], sws_sem.at[chunk], swr_sem.at[chunk], (dp, partner)
        )

    for chunk in range(2):
        slots_self(s_send, s_recv, self_sem, chunk).wait()
        for i in range(1, 8):
            slots_wait(s_send, s_recv, ds_sem, dr_sem, chunk, i)
        slot_grads(chunk)
        start([swap_copy(chunk)])
        start([slots_copy(sg_v, ret_v, rs_sem, rr_sem, chunk, i) for i in range(1, 8)])
        slots_self(sg_v, ret_v, ret_self_sem, chunk).start()

    def down_block(q, carry):
        cols = pl.ds(pl.multiple_of(q * 256, 256), 256)
        left = s_recv[:, :, cols].reshape(256, 256)
        out = lax.dot_general(left, hid_v[...].reshape(256, 512), TN, preferred_element_type=F32)
        keep(0, q, out)
        return carry

    def both_block(q, carry):
        cols = pl.ds(pl.multiple_of(q * 256, 256), 256)
        left = x_v[:, :, :, cols].reshape(512, 256)
        out = lax.dot_general(left, dg_v[...].reshape(512, 512), TN, preferred_element_type=F32)
        keep(1, q, out)
        return carry

    def keep(g, q, out):
        out = out.reshape(4, 2, 32, 512)
        at = pl.ds(4 * (q % 2), 4)
        rf[g, q // 2, at] = out
        rb[g, q // 2, at] = out.astype(BF16)

    def core_copy(g):
        return remote(rb.at[g, :, :, 1 - core], drecv.at[g], cs_sem.at[g], cr_sem.at[g], (dp_core, mem))

    def term(g, owner):
        return rf[g, :, owner, core] + drecv[g, :, owner].astype(F32)

    def long_copy(g, t):
        return remote(lsend.at[g, t], lrecv.at[g, t], lss_sem.at[g, t], lsr_sem.at[g, t], (dp_fwd, mem))

    def short_copy(g, t):
        return remote(ssend.at[g, t], srecv.at[g, t], sss_sem.at[g, t], ssr_sem.at[g, t], (dp_bwd, mem))

    def ring_first(g):
        core_copy(g).wait_recv()
        lsend[g, 0] = term(g, (y + 4) % 8).astype(BF16)
        start([long_copy(g, 0)])
        ssend[g, 0] = term(g, (y - 3 * step + 8) % 8).astype(BF16)
        start([short_copy(g, 0)])

    def ring_next(g, t):
        own = term(g, (y + (4 - t) * step + 8) % 8)
        long_copy(g, t - 1).wait_recv()
        lsend[g, t] = (own + lrecv[g, t - 1].astype(F32)).astype(BF16)
        start([long_copy(g, t)])
        if t < 3:
            own = term(g, (y - (3 - t) * step + 8) % 8)
            short_copy(g, t - 1).wait_recv()
            ssend[g, t] = (own + srecv[g, t - 1].astype(F32)).astype(BF16)
            start([short_copy(g, t)])

    def ring_last(g):
        own = term(g, y)
        short_copy(g, 2).wait_recv()
        own = own + srecv[g, 2].astype(F32)
        long_copy(g, 3).wait_recv()
        own = own + lrecv[g, 3].astype(F32)
        fin[g] = own
        finb[g] = own.astype(BF16)

    def z_copies(g):
        if g == 1:
            return [remote(finb.at[1, 1 - zl], z1, zs_sem.at[3], zr_sem.at[3], (dp_z, mem))]
        own, other = pl.ds(0, 256), pl.ds(256, 256)
        return [
            remote(finb.at[0, 1 - zl, :, own], zd.at[0], zs_sem.at[0], zr_sem.at[0], (dp_z, mem)),
            remote(finb.at[0, zl, :, other], zd.at[1], zs_sem.at[1], zr_sem.at[1], (dp, partner)),
            remote(finb.at[0, 1 - zl, :, other], zd.at[2], zs_sem.at[2], zr_sem.at[2], (dp_z, partner)),
        ]

    lax.fori_loop(0, 4, down_block, 0)
    start([core_copy(0)])
    for chunk in range(2):
        swap_copy(chunk).wait_recv()
    ring_first(0)
    lax.fori_loop(0, 4, both_block, 0)
    start([core_copy(1)])

    def tokens(chunk):
        slots_self(sg_v, ret_v, ret_self_sem, chunk).wait()
        for i in range(1, 8):
            slots_wait(sg_v, ret_v, rs_sem, rr_sem, chunk, i)
        for mb in (2 * chunk, 2 * chunk + 1):
            gin_ref[mb] = jnp.dot(mix_v[mb], ret_v[mb], preferred_element_type=F32).astype(BF16)

    ring_first(1)
    ring_next(0, 1)
    ring_next(1, 1)
    tokens(0)
    ring_next(0, 2)
    ring_next(1, 2)
    ring_next(0, 3)
    ring_next(1, 3)
    tokens(1)
    ring_last(0)
    start(z_copies(0))
    ring_last(1)
    start(z_copies(1))

    scale = 1.0 / 128.0
    for copy in z_copies(0):
        copy.wait_recv()
    down = fin[0, zl, :, pl.ds(0, 256)]
    for n in range(3):
        down = down + zd[n].astype(F32)
    gd_ref[...] = down * scale
    for copy in z_copies(1):
        copy.wait_recv()
    both = (fin[1, zl] + z1[...].astype(F32)) * scale
    gg_ref[...] = both[:, :256]
    gu_ref[...] = both[:, 256:]

    for copy in sends:
        copy.wait_send()


def per_device(grad_out, routes, route_probs, dispatched, w_gate, w_up, w_down):
    wg = w_gate.reshape(2, 4, 2, 64, 256)
    wu = w_up.reshape(2, 4, 2, 64, 256)
    wd = w_down.reshape(2, 4, 2, 16, 1024)
    hbm = pl.BlockSpec(memory_space=pl.ANY)
    vmem = pl.BlockSpec(memory_space=pltpu.VMEM)
    dma = pltpu.SemaphoreType.DMA
    V = pltpu.VMEM
    return pl.pallas_call(
        kernel,
        out_shape=(
            jax.ShapeDtypeStruct((4, 64, 1024), BF16),
            jax.ShapeDtypeStruct((32, 256), F32),
            jax.ShapeDtypeStruct((32, 256), F32),
            jax.ShapeDtypeStruct((32, 256), F32),
        ),
        in_specs=[hbm] * 7,
        out_specs=(vmem,) * 4,
        scratch_shapes=[
            V((4, 64, 8), jnp.int32),
            V((4, 64, 8), BF16),
            V((4, 64, 1024), BF16),
            V((2, 4, 64, 1024), BF16),
            V((2, 4, 2, 64, 512), BF16),
            V((2, 4, 2, 16, 1024), BF16),
            V((2, 4, 2, 64, 512), BF16),
            V((2, 4, 2, 16, 1024), BF16),
            V((4, 64, 64), BF16),
            V((4, 64, 1024), BF16),
            V((4, 64, 1024), BF16),
            V((2, 2, 128, 256), F32),
            V((2, 2, 128, 256), F32),
            V((2, 128, 512), BF16),
            V((2, 2, 128, 512), BF16),
            V((2, 128, 512), BF16),
            V((4, 64, 1024), BF16),
            V((4, 64, 1024), BF16),
            V((2, 2, 8, 2, 32, 512), F32),
            V((2, 2, 8, 2, 32, 512), BF16),
            V((2, 2, 8, 32, 512), BF16),
            V((2, 4, 2, 32, 512), BF16),
            V((2, 4, 2, 32, 512), BF16),
            V((2, 3, 2, 32, 512), BF16),
            V((2, 3, 2, 32, 512), BF16),
            V((2, 2, 32, 512), F32),
            V((2, 2, 32, 512), BF16),
            V((32, 512), BF16),
            V((3, 32, 256), BF16),
            dma((6,)), dma((2, 8)), dma((2,)), dma((2,)),
            dma((2, 7)), dma((2, 7)), dma((2, 7)), dma((2, 7)),
            dma((8, 2)), dma((8, 2)), dma((2,)), dma((2,)), dma((2,)), dma((2,)),
            dma((2, 4)), dma((2, 4)), dma((2, 3)), dma((2, 3)), dma((4,)), dma((4,)),
        ],
        compiler_params=pltpu.CompilerParams(
            collective_id=0, has_side_effects=True, vmem_limit_bytes=48 * 1024 * 1024
        ),
        name="moe_backward",
    )(grad_out, routes, route_probs, dispatched, wg, wu, wd)


def solution(mesh):
    return jax.shard_map(
        per_device,
        mesh=mesh,
        in_specs=(
            P(None, ("dp", "expert"), None),
            P(None, ("dp", "expert"), None),
            P(None, ("dp", "expert"), None),
            P(None, ("dp", "expert"), None),
            P(None, "expert"),
            P(None, "expert"),
            P("expert", None),
        ),
        out_specs=(
            P(None, ("dp", "expert"), None),
            P("dp", "expert"),
            P("dp", "expert"),
            P("dp", "expert"),
        ),
        check_vma=False,
    )
```

```python
import jax
import jax.numpy as jnp
from jax import lax
from jax.experimental import pallas as pl
from jax.experimental.pallas import tpu as pltpu
from jax.sharding import PartitionSpec as P

MESH = pl.DeviceIdType.MESH
F32 = jnp.float32
BF16 = jnp.bfloat16

NT = (((1,), (1,)), ((), ()))
TN = (((0,), (0,)), ((), ()))


def kernel(
    dy_hbm, routes_hbm, probs_hbm, disp_hbm, wg_hbm, wu_hbm, wd_hbm,
    gin_hbm, gg_hbm, gu_hbm, gd_hbm,
    routes_v, probs_v, dy_v, x_v, wgu, wd, pgu, pd,
    mix_v, s_send, s_recv, act_v, fac_v, hid_v, dg_v, sg_v, ret_v,
    rf, rb, drecv, lsend, lrecv, ssend, srecv, fin, finb, zd, gin_v, gate_v, up_v, down_v,
    in_sem, x_sem, out_sem, self_sem, ret_self_sem,
    ds_sem, dr_sem, rs_sem, rr_sem,
    ws_sem, wr_sem, cs_sem, cr_sem,
    lss_sem, lsr_sem, sss_sem, ssr_sem, zs_sem, zr_sem,
):
    dp = lax.axis_index("dp")
    mem = lax.axis_index("expert")
    core = dp % 2
    y = (dp // 2) % 8
    zl = dp // 16
    step = 1 - 2 * core
    mine = mem // 2
    zh = mem % 4
    low = (zh * (3 - zh)) // 2

    def peer_of(e):
        return 4 * (e // 2) + low + (e % 2) * (3 - 2 * low)

    partner = mem + 1 - 2 * (mem % 2)
    dp_core = dp + 1 - 2 * core
    dp_fwd = zl * 16 + ((y + step + 8) % 8) * 2 + core
    dp_bwd = zl * 16 + ((y - step + 8) % 8) * 2 + core
    dp_z = (1 - zl) * 16 + y * 2 + core

    def remote(src, dst, ssem, rsem, dev):
        return pltpu.make_async_remote_copy(
            src_ref=src, dst_ref=dst, send_sem=ssem, recv_sem=rsem,
            device_id=dev, device_id_type=MESH,
        )

    barrier = pltpu.get_barrier_semaphore()
    peers = [(dp, peer_of((mine + i) % 8)) for i in range(1, 8)]
    peers += [(dp, partner), (dp_core, mem), (dp_fwd, mem), (dp_bwd, mem), (dp_z, mem), (dp_z, partner)]
    for dev in peers:
        pl.semaphore_signal(barrier, inc=1, device_id=dev, device_id_type=MESH)

    loads = [
        pltpu.make_async_copy(wg_hbm, wgu.at[:, :, :, :, pl.ds(0, 256)], in_sem.at[3]),
        pltpu.make_async_copy(wu_hbm, wgu.at[:, :, :, :, pl.ds(256, 256)], in_sem.at[4]),
        pltpu.make_async_copy(wd_hbm, wd, in_sem.at[5]),
        pltpu.make_async_copy(routes_hbm, routes_v, in_sem.at[0]),
        pltpu.make_async_copy(probs_hbm, probs_v, in_sem.at[1]),
        pltpu.make_async_copy(dy_hbm, dy_v, in_sem.at[2]),
    ]
    for load in loads:
        load.start()
    with jax.named_scope("barrier"):
        for load in loads[:3]:
            load.wait()
        pl.semaphore_wait(barrier, len(peers))

    sends = []
    quarter = y % 4

    def weights_copy(n, h, src_a, src_b, where, side, dev, come=None):
        come = n if come is None else come
        return [
            remote(
                src_a.at[h, where, side], pgu.at[h, where, side], ws_sem.at[n, h, 0], wr_sem.at[come, h, 0], dev
            ),
            remote(
                src_b.at[h, where, side], pd.at[h, where, side], ws_sem.at[n, h, 1], wr_sem.at[come, h, 1], dev
            ),
        ]

    def start(copies):
        for copy in copies:
            copy.start()
        sends.extend(copies)

    def weights_wait(n, h, where, side):
        for copy in weights_copy(n, h, pgu, pd, where, side, (dp_core, mem)):
            copy.wait_recv()

    def pass_on(n, h, where, dev):
        start(weights_copy(n, h, pgu, pd, where, core, dev))

    near = (zl + zh) % 2 == 1
    far = (zl + zh) % 2 == 0
    near_sends = []
    for h in range(2):
        near_sends += weights_copy(0, h, wgu, wd, quarter, core, (dp_z, partner))

    @pl.when(near)
    def _():
        for copy in near_sends:
            copy.start()

    with jax.named_scope("wait_in"):
        for load in loads[3:]:
            load.wait()

    def route(mb, carry):
        ids = routes_v[mb]
        probs = probs_v[mb].astype(F32)
        lane = lax.broadcasted_iota(jnp.int32, (64, 64), 1)
        row = lax.broadcasted_iota(jnp.int32, (64, 64), 0)
        expert = lax.shift_right_logical(row, 3)
        place = lax.bitwise_and(row, 7)
        hit = jnp.zeros((64, 64), F32)
        weight = jnp.zeros((64, 64), F32)
        for k in range(8):
            same = ids[k : k + 1, :] == expert
            hit = hit + jnp.where(same, 1.0, 0.0)
            weight = weight + jnp.where(same, probs[k : k + 1, :], 0.0)
        earlier = jnp.where(row < lane, 1.0, 0.0).astype(BF16)
        rank = jnp.dot(hit.astype(BF16), earlier, preferred_element_type=F32)
        chosen = jnp.where(rank == place.astype(F32), hit, 0.0)
        mix_v[mb] = chosen.astype(BF16)
        weighted = (chosen * weight).astype(BF16)
        scaled = jnp.dot(weighted, dy_v[mb], preferred_element_type=F32)
        s_send[mb] = scaled.astype(BF16)
        return carry

    x_loads = []
    for j in range(8):
        src = 4 * (j // 2) + (low if j % 2 == 0 else 3 - low)
        x_loads.append(
            pltpu.make_async_copy(
                disp_hbm.at[:, pl.ds(pl.multiple_of(src * 8, 8), 8)],
                x_v.at[:, pl.ds(j * 8, 8)],
                x_sem.at[j],
            )
        )
    for load in x_loads:
        load.start()
    with jax.named_scope("route"):
        lax.fori_loop(0, 4, route, 0)
    def slots_copy(src, dst, sem_s, sem_r, chunk, i):
        to = (mine + i) % 8
        return remote(
            src.at[pl.ds(2 * chunk, 2), pl.ds(pl.multiple_of(to * 8, 8), 8)],
            dst.at[pl.ds(2 * chunk, 2), pl.ds(pl.multiple_of(mine * 8, 8), 8)],
            sem_s.at[chunk, i - 1],
            sem_r.at[chunk, i - 1],
            (dp, peer_of(to)),
        )

    def slots_wait(src, dst, sem_s, sem_r, chunk, i):
        came = (mine + 8 - i) % 8
        remote(
            src.at[pl.ds(2 * chunk, 2), pl.ds(pl.multiple_of(came * 8, 8), 8)],
            dst.at[pl.ds(2 * chunk, 2), pl.ds(pl.multiple_of(came * 8, 8), 8)],
            sem_s.at[chunk, i - 1],
            sem_r.at[chunk, i - 1],
            (dp, peer_of((mine + i) % 8)),
        ).wait_recv()

    def slots_self(src, dst, sem, chunk):
        at = pl.ds(pl.multiple_of(mine * 8, 8), 8)
        return pltpu.make_async_copy(
            src.at[pl.ds(2 * chunk, 2), at], dst.at[pl.ds(2 * chunk, 2), at], sem.at[chunk]
        )

    crossing = [slots_copy(s_send, s_recv, ds_sem, dr_sem, chunk, i) for chunk in range(2) for i in (1, 3, 5, 7)]
    for chunk in range(2):
        start([slots_copy(s_send, s_recv, ds_sem, dr_sem, chunk, i) for i in (2, 4, 6)])
        slots_self(s_send, s_recv, self_sem, chunk).start()
    sends.extend(crossing)

    @pl.when(far)
    def _():
        for copy in crossing:
            copy.start()

    with jax.named_scope("wait_x"):
        for load in x_loads:
            load.wait()

    def hidden(half, weights):
        def body(chunk, carry):
            rows = x_v[pl.ds(2 * chunk, 2)].reshape(128, 1024)
            both = jnp.dot(rows, weights[...].reshape(1024, 512), preferred_element_type=F32)
            gate, up = both[:, :256], both[:, 256:]
            sig = jax.nn.sigmoid(gate)
            act = gate * sig
            act_v[half, chunk] = act
            fac_v[half, chunk] = up * sig * (1.0 + gate * (1.0 - sig))
            hid_v[chunk, :, pl.ds(256 * half, 256)] = (act * up).astype(BF16)
            return carry

        lax.fori_loop(0, 2, body, 0)

    def d_terms(half, chunk, down):
        rows = s_recv[pl.ds(2 * chunk, 2)].reshape(128, 1024)
        dh = lax.dot_general(rows, down[...].reshape(256, 1024), NT, preferred_element_type=F32)
        d_both = jnp.concatenate(
            [(dh * fac_v[half, chunk]).astype(BF16), (dh * act_v[half, chunk]).astype(BF16)], axis=1
        )
        dg_v[half, chunk] = d_both

    def slot_grads(chunk):
        total = lax.dot_general(
            dg_v[0, chunk], wgu[...].reshape(1024, 512), NT, preferred_element_type=F32
        ) + lax.dot_general(dg_v[1, chunk], pgu[...].reshape(1024, 512), NT, preferred_element_type=F32)
        sg_v[pl.ds(2 * chunk, 2)] = total.astype(BF16).reshape(2, 64, 1024)

    def weight_terms(half, s):
        z = (zl + 1 + s) % 2

        def body(q, carry):
            cols = pl.ds(pl.multiple_of((2 * z + q) * 256, 256), 256)
            at = pl.ds(4 * q, 4)
            right = hid_v[:, :, pl.ds(256 * half, 256)].reshape(256, 256)
            out = lax.dot_general(s_recv[:, :, cols].reshape(256, 256), right, TN, preferred_element_type=F32)
            out = out.reshape(4, 2, 32, 256)
            rf[half, s, at, :, :, pl.ds(0, 256)] = out
            rb[half, s, at, :, :, pl.ds(0, 256)] = out.astype(BF16)
            right = dg_v[half].reshape(256, 512)
            out = lax.dot_general(x_v[:, :, cols].reshape(256, 256), right, TN, preferred_element_type=F32)
            out = out.reshape(4, 2, 32, 512)
            rf[half, s, at, :, :, pl.ds(256, 512)] = out
            rb[half, s, at, :, :, pl.ds(256, 512)] = out.astype(BF16)
            return carry

        lax.fori_loop(0, 2, body, 0)
        start([core_copy(half, s)])

    def core_copy(g, s):
        return remote(rb.at[g, s, :, 1 - core], drecv.at[g, s], cs_sem.at[g, s], cr_sem.at[g, s], (dp_core, mem))

    def term(g, s, owner):
        return rf[g, s, owner, core] + drecv[g, s, owner].astype(F32)

    def long_copy(g, s, t):
        at = (g, s, t)
        return remote(lsend.at[at], lrecv.at[at], lss_sem.at[at], lsr_sem.at[at], (dp_fwd, mem))

    def short_copy(g, s, t):
        at = (g, s, t)
        return remote(ssend.at[at], srecv.at[at], sss_sem.at[at], ssr_sem.at[at], (dp_bwd, mem))

    def ring_first(g, s):
        core_copy(g, s).wait_recv()
        lsend[g, s, 0] = term(g, s, (y + 4) % 8).astype(BF16)
        start([long_copy(g, s, 0)])
        ssend[g, s, 0] = term(g, s, (y - 3 * step + 8) % 8).astype(BF16)
        start([short_copy(g, s, 0)])

    def ring_next(g, s, t):
        own = term(g, s, (y + (4 - t) * step + 8) % 8)
        long_copy(g, s, t - 1).wait_recv()
        lsend[g, s, t] = (own + lrecv[g, s, t - 1].astype(F32)).astype(BF16)
        start([long_copy(g, s, t)])
        if t < 3:
            own = term(g, s, (y - (3 - t) * step + 8) % 8)
            short_copy(g, s, t - 1).wait_recv()
            ssend[g, s, t] = (own + srecv[g, s, t - 1].astype(F32)).astype(BF16)
            start([short_copy(g, s, t)])

    def z_copy(g, s):
        n = (0, None, 1, 2)[2 * g + s]
        dev = ((dp_z, dp)[s], (mem, partner)[g])
        return remote(finb.at[g, s], zd.at[n], zs_sem.at[n], zr_sem.at[n], dev)

    def ring_last(g, s):
        own = term(g, s, y)
        short_copy(g, s, 2).wait_recv()
        own = own + srecv[g, s, 2].astype(F32)
        long_copy(g, s, 3).wait_recv()
        own = own + lrecv[g, s, 3].astype(F32)
        if g == 0 and s == 1:
            fin[...] = own
        else:
            finb[g, s] = own.astype(BF16)
            start([z_copy(g, s)])

    def slots_arrive(chunk):
        slots_self(s_send, s_recv, self_sem, chunk).wait()
        for i in range(1, 8):
            slots_wait(s_send, s_recv, ds_sem, dr_sem, chunk, i)

    from_bwd = (y - step + 8) % 4
    from_fwd = (y + step + 8) % 4
    across = (y + 2) % 4

    def first_piece(h):
        weights_wait(0, h, quarter, core)
        relays = weights_copy(8, h, pgu, pd, quarter, core, (dp_z, mem), 0)
        near_sends.extend(relays)

        @pl.when(near)
        def _():
            for copy in relays:
                copy.start()

        pass_on(1, h, quarter, (dp_fwd, mem))
        pass_on(2, h, quarter, (dp_bwd, mem))
        pass_on(4, h, quarter, (dp_core, mem))

    def second_piece(h):
        weights_wait(1, h, from_bwd, core)
        pass_on(3, h, from_bwd, (dp_fwd, mem))
        pass_on(5, h, from_bwd, (dp_core, mem))
        weights_wait(2, h, from_fwd, core)
        pass_on(6, h, from_fwd, (dp_core, mem))

    def third_piece(h):
        weights_wait(3, h, across, core)
        pass_on(7, h, across, (dp_core, mem))

    def last_piece(h):
        weights_wait(4, h, quarter, 1 - core)
        weights_wait(5, h, from_fwd, 1 - core)
        weights_wait(6, h, from_bwd, 1 - core)
        weights_wait(7, h, across, 1 - core)

    stores = []

    def store(src, dst, n):
        copy = pltpu.make_async_copy(src, dst, out_sem.at[n])
        copy.start()
        stores.append(copy)

    def tokens(chunk):
        slots_self(sg_v, ret_v, ret_self_sem, chunk).wait()
        for i in range(1, 8):
            slots_wait(sg_v, ret_v, rs_sem, rr_sem, chunk, i)
        for mb in (2 * chunk, 2 * chunk + 1):
            gin_v[mb] = lax.dot_general(mix_v[mb], ret_v[mb], TN, preferred_element_type=F32).astype(BF16)
        half = pl.ds(2 * chunk, 2)
        store(gin_v.at[half], gin_hbm.at[half], chunk)

    with jax.named_scope("hidden0"):
        hidden(0, wgu)
    with jax.named_scope("w0a"):
        first_piece(0)
    with jax.named_scope("w0b"):
        first_piece(1)

    @pl.when(near)
    def _():
        for copy in crossing:
            copy.start()

    with jax.named_scope("w1a"):
        second_piece(0)
    with jax.named_scope("w1b"):
        second_piece(1)
    with jax.named_scope("w3a"):
        third_piece(0)
    with jax.named_scope("slots0"):
        slots_arrive(0)
    with jax.named_scope("d_own0"):
        d_terms(0, 0, wd)
    with jax.named_scope("w3b"):
        third_piece(1)
    with jax.named_scope("slots1"):
        slots_arrive(1)
    with jax.named_scope("d_own1"):
        d_terms(0, 1, wd)
    with jax.named_scope("weights0"):
        weight_terms(0, 0)
        weight_terms(0, 1)
    with jax.named_scope("ring_first0"):
        ring_first(0, 0)
        ring_first(0, 1)
    with jax.named_scope("wlast"):
        last_piece(0)
        last_piece(1)
    with jax.named_scope("hidden1"):
        hidden(1, pgu)
    with jax.named_scope("d_partner"):
        d_terms(1, 0, pd)
        d_terms(1, 1, pd)
    with jax.named_scope("ring_next0_1a"):
        ring_next(0, 0, 1)
    with jax.named_scope("slot_grads0"):
        slot_grads(0)
        start([slots_copy(sg_v, ret_v, rs_sem, rr_sem, 0, i) for i in range(1, 8)])
        slots_self(sg_v, ret_v, ret_self_sem, 0).start()
    with jax.named_scope("weights1"):
        weight_terms(1, 0)
        weight_terms(1, 1)
    with jax.named_scope("ring_next0_1b"):
        ring_next(0, 1, 1)
    with jax.named_scope("slot_grads1"):
        slot_grads(1)
        start([slots_copy(sg_v, ret_v, rs_sem, rr_sem, 1, i) for i in range(1, 8)])
        slots_self(sg_v, ret_v, ret_self_sem, 1).start()
    with jax.named_scope("ring_first1"):
        ring_first(1, 0)
        ring_first(1, 1)
    with jax.named_scope("ring_next0_2"):
        ring_next(0, 0, 2)
        ring_next(0, 1, 2)
    with jax.named_scope("ring_next1_1"):
        ring_next(1, 0, 1)
        ring_next(1, 1, 1)
    with jax.named_scope("ring_next0_3"):
        ring_next(0, 0, 3)
        ring_next(0, 1, 3)
    with jax.named_scope("ring_next1_2"):
        ring_next(1, 0, 2)
        ring_next(1, 1, 2)
    with jax.named_scope("ring_last0"):
        ring_last(0, 0)
        ring_last(0, 1)
    with jax.named_scope("tokens0"):
        tokens(0)
    with jax.named_scope("ring_next1_3"):
        ring_next(1, 0, 3)
        ring_next(1, 1, 3)
    with jax.named_scope("tokens1"):
        tokens(1)
    with jax.named_scope("ring_last1"):
        ring_last(1, 0)
        ring_last(1, 1)

    with jax.named_scope("wait_z"):
        for copy in (z_copy(0, 0), z_copy(1, 0), z_copy(1, 1)):
            copy.wait_recv()
    total = fin[...]
    for n in range(3):
        total = total + zd[n].astype(F32)
    total = total * (1.0 / 128.0)
    down_v[...] = total[:, :256]
    store(down_v, gd_hbm, 2)
    gate_v[...] = total[:, 256:512]
    store(gate_v, gg_hbm, 3)
    up_v[...] = total[:, 512:]
    store(up_v, gu_hbm, 4)

    with jax.named_scope("wait_sends"):
        for copy in sends:
            copy.wait_send()
        for copy in stores:
            copy.wait()

        @pl.when(near)
        def _():
            for copy in near_sends:
                copy.wait_send()


def per_device(grad_out, routes, route_probs, dispatched, w_gate, w_up, w_down):
    wg = w_gate.reshape(2, 4, 2, 64, 256)
    wu = w_up.reshape(2, 4, 2, 64, 256)
    wd = w_down.reshape(2, 4, 2, 16, 1024)
    hbm = pl.BlockSpec(memory_space=pltpu.HBM)
    vmem = pl.BlockSpec(memory_space=pltpu.VMEM)
    dma = pltpu.SemaphoreType.DMA
    V = pltpu.VMEM
    results = pl.pallas_call(
        kernel,
        out_shape=(
            jax.ShapeDtypeStruct((4, 64, 1024), BF16),
            jax.ShapeDtypeStruct((32, 256), F32),
            jax.ShapeDtypeStruct((32, 256), F32),
            jax.ShapeDtypeStruct((32, 256), F32),
        ),
        in_specs=[hbm] * 7,
        out_specs=(hbm,) * 4,
        scratch_shapes=[
            V((4, 8, 64), jnp.int32),
            V((4, 8, 64), BF16),
            V((4, 64, 1024), BF16),
            V((4, 64, 1024), BF16),
            V((2, 4, 2, 64, 512), BF16),
            V((2, 4, 2, 16, 1024), BF16),
            V((2, 4, 2, 64, 512), BF16),
            V((2, 4, 2, 16, 1024), BF16),
            V((4, 64, 64), BF16),
            V((4, 64, 1024), BF16),
            V((4, 64, 1024), BF16),
            V((2, 2, 128, 256), F32),
            V((2, 2, 128, 256), F32),
            V((2, 128, 512), BF16),
            V((2, 2, 128, 512), BF16),
            V((4, 64, 1024), BF16),
            V((4, 64, 1024), BF16),
            V((2, 2, 8, 2, 32, 768), F32),
            V((2, 2, 8, 2, 32, 768), BF16),
            V((2, 2, 8, 32, 768), BF16),
            V((2, 2, 4, 32, 768), BF16),
            V((2, 2, 4, 32, 768), BF16),
            V((2, 2, 3, 32, 768), BF16),
            V((2, 2, 3, 32, 768), BF16),
            V((32, 768), F32),
            V((2, 2, 32, 768), BF16),
            V((3, 32, 768), BF16),
            V((4, 64, 1024), BF16),
            V((32, 256), F32),
            V((32, 256), F32),
            V((32, 256), F32),
            dma((6,)), dma((8,)), dma((5,)), dma((2,)), dma((2,)),
            dma((2, 7)), dma((2, 7)), dma((2, 7)), dma((2, 7)),
            dma((9, 2, 2)), dma((8, 2, 2)), dma((2, 2)), dma((2, 2)),
            dma((2, 2, 4)), dma((2, 2, 4)), dma((2, 2, 3)), dma((2, 2, 3)), dma((3,)), dma((3,)),
        ],
        compiler_params=pltpu.CompilerParams(
            collective_id=0, has_side_effects=True, vmem_limit_bytes=62000000
        ),
        name="moe_backward",
    )(grad_out, jnp.swapaxes(routes, 1, 2), jnp.swapaxes(route_probs, 1, 2), dispatched, wg, wu, wd)

    def store(a, b, c, d, out_a, out_b, out_c, out_d, sem):
        copies = [
            pltpu.make_async_copy(src, dst, sem.at[n])
            for n, (src, dst) in enumerate(((a, out_a), (b, out_b), (c, out_c), (d, out_d)))
        ]
        for copy in copies:
            copy.start()
        for copy in copies:
            copy.wait()

    return pl.pallas_call(
        store,
        out_shape=tuple(jax.ShapeDtypeStruct(r.shape, r.dtype) for r in results),
        in_specs=[vmem] * 4,
        out_specs=(hbm,) * 4,
        scratch_shapes=[dma((4,))],
        name="store_results",
    )(*results)


def solution(mesh):
    return jax.shard_map(
        per_device,
        mesh=mesh,
        in_specs=(
            P(None, ("dp", "expert"), None),
            P(None, ("dp", "expert"), None),
            P(None, ("dp", "expert"), None),
            P(None, ("dp", "expert"), None),
            P(None, "expert"),
            P(None, "expert"),
            P("expert", None),
        ),
        out_specs=(
            P(None, ("dp", "expert"), None),
            P("dp", "expert"),
            P("dp", "expert"),
            P("dp", "expert"),
        ),
        check_vma=False,
    )
```

```python
import jax
import jax.numpy as jnp
from jax import lax
from jax.experimental import pallas as pl
from jax.experimental.pallas import tpu as pltpu
from jax.sharding import PartitionSpec as P

MESH = pl.DeviceIdType.MESH
F32 = jnp.float32
BF16 = jnp.bfloat16

NT = (((1,), (1,)), ((), ()))
TN = (((0,), (0,)), ((), ()))


def kernel(
    dy_hbm, routes_hbm, probs_hbm, disp_hbm, wg_hbm, wu_hbm, wd_hbm,
    gin_v, gate_v, up_v, down_v,
    routes_v, probs_v, dy_v, x_v, wgu, wd, pgu, pd,
    mix_v, s_send, s_recv, act_v, fac_v, hid_v, dg_v, sg_v, ret_v,
    rf, rb, drecv, lsend, lrecv, ssend, srecv, fin, finb, zd,
    in_sem, x_sem,
    ds_sem, dr_sem, rs_sem, rr_sem,
    ws_sem, wr_sem, cs_sem, cr_sem,
    lsr_sem, ssr_sem, zr_sem,
):
    dp = lax.axis_index("dp")
    mem = lax.axis_index("expert")
    core = dp % 2
    y = (dp // 2) % 8
    zl = dp // 16
    step = 1 - 2 * core
    mine = mem // 2
    zh = mem % 4
    low = (zh * (3 - zh)) // 2

    def peer_of(e):
        return 4 * (e // 2) + low + (e % 2) * (3 - 2 * low)

    partner = mem + 1 - 2 * (mem % 2)
    dp_core = dp + 1 - 2 * core
    dp_fwd = zl * 16 + ((y + step + 8) % 8) * 2 + core
    dp_bwd = zl * 16 + ((y - step + 8) % 8) * 2 + core
    dp_z = (1 - zl) * 16 + y * 2 + core

    def remote(src, dst, ssem, rsem, dev):
        return pltpu.make_async_remote_copy(
            src_ref=src, dst_ref=dst, send_sem=ssem, recv_sem=rsem,
            device_id=dev, device_id_type=MESH,
        )

    barrier = pltpu.get_barrier_semaphore()
    peers = [(dp, peer_of((mine + i) % 8)) for i in range(1, 8)]
    peers += [(dp, partner), (dp_core, mem), (dp_fwd, mem), (dp_bwd, mem), (dp_z, mem), (dp_z, partner)]
    for dev in peers:
        pl.semaphore_signal(barrier, inc=1, device_id=dev, device_id_type=MESH)

    loads = [
        pltpu.make_async_copy(wg_hbm, wgu.at[:, :, :, :, pl.ds(0, 256)], in_sem.at[3]),
        pltpu.make_async_copy(wu_hbm, wgu.at[:, :, :, :, pl.ds(256, 256)], in_sem.at[4]),
        pltpu.make_async_copy(wd_hbm, wd, in_sem.at[5]),
        pltpu.make_async_copy(routes_hbm, routes_v, in_sem.at[0]),
        pltpu.make_async_copy(probs_hbm, probs_v, in_sem.at[1]),
        pltpu.make_async_copy(dy_hbm, dy_v, in_sem.at[2]),
    ]
    for load in loads:
        load.start()
    with jax.named_scope("barrier"):
        for load in loads[:3]:
            load.wait()
        pl.semaphore_wait(barrier, len(peers))

    quarter = y % 4

    def weights_copy(n, h, src_a, src_b, where, side, dev, come=None):
        come = n if come is None else come
        kind = 0 if 0 < n < 8 else 1
        return [
            remote(src_a.at[h, where, side], pgu.at[h, where, side], ws_sem.at[kind, 0], wr_sem.at[come, h, 0], dev),
            remote(src_b.at[h, where, side], pd.at[h, where, side], ws_sem.at[kind, 1], wr_sem.at[come, h, 1], dev),
        ]

    def start(copies):
        for copy in copies:
            copy.start()

    def weights_wait(n, h, where, side):
        for copy in weights_copy(n, h, pgu, pd, where, side, (dp_core, mem)):
            copy.wait_recv()

    def pass_on(n, h, where, dev):
        start(weights_copy(n, h, pgu, pd, where, core, dev))

    near = (zl + zh) % 2 == 1
    far = (zl + zh) % 2 == 0
    near_sends = []
    for h in range(2):
        near_sends += weights_copy(0, h, wgu, wd, quarter, core, (dp_z, partner))

    @pl.when(near)
    def _():
        for copy in near_sends:
            copy.start()

    with jax.named_scope("wait_in"):
        for load in loads[3:]:
            load.wait()

    def route(mb, carry):
        ids = routes_v[mb]
        probs = probs_v[mb].astype(F32)
        lane = lax.broadcasted_iota(jnp.int32, (64, 64), 1)
        row = lax.broadcasted_iota(jnp.int32, (64, 64), 0)
        expert = lax.shift_right_logical(row, 3)
        place = lax.bitwise_and(row, 7)
        hit = jnp.zeros((64, 64), F32)
        weight = jnp.zeros((64, 64), F32)
        for k in range(8):
            same = ids[k : k + 1, :] == expert
            hit = hit + jnp.where(same, 1.0, 0.0)
            weight = weight + jnp.where(same, probs[k : k + 1, :], 0.0)
        earlier = jnp.where(row < lane, 1.0, 0.0).astype(BF16)
        rank = jnp.dot(hit.astype(BF16), earlier, preferred_element_type=F32)
        chosen = jnp.where(rank == place.astype(F32), hit, 0.0)
        mix_v[mb] = chosen.astype(BF16)
        weighted = (chosen * weight).astype(BF16)
        scaled = jnp.dot(weighted, dy_v[mb], preferred_element_type=F32)
        s_send[mb] = scaled.astype(BF16)
        return carry

    x_loads = []
    for j in range(8):
        src = 4 * (j // 2) + (low if j % 2 == 0 else 3 - low)
        x_loads.append(
            pltpu.make_async_copy(
                disp_hbm.at[:, pl.ds(pl.multiple_of(src * 8, 8), 8)],
                x_v.at[:, pl.ds(j * 8, 8)],
                x_sem.at[0],
            )
        )
    for load in x_loads:
        load.start()
    def slots_copy(src, dst, sem_s, sem_r, chunk, i):
        to = (mine + i) % 8
        return remote(
            src.at[pl.ds(2 * chunk, 2), pl.ds(pl.multiple_of(to * 8, 8), 8)],
            dst.at[pl.ds(2 * chunk, 2), pl.ds(pl.multiple_of(mine * 8, 8), 8)],
            sem_s.at[0],
            sem_r.at[chunk],
            (dp, peer_of(to)),
        )

    def slots_self(src, dst, sem_r, chunk):
        at = pl.ds(pl.multiple_of(mine * 8, 8), 8)
        return pltpu.make_async_copy(
            src.at[pl.ds(2 * chunk, 2), at], dst.at[pl.ds(2 * chunk, 2), at], sem_r.at[chunk]
        )

    def slots_wait(dst, sem_r, chunk):
        rows = dst.at[pl.ds(2 * chunk, 2)]
        pltpu.make_async_copy(rows, rows, sem_r.at[chunk]).wait()

    crossing = []
    for chunk in range(2):
        with jax.named_scope("route"):
            lax.fori_loop(2 * chunk, 2 * chunk + 2, route, 0)
        start([slots_copy(s_send, s_recv, ds_sem, dr_sem, chunk, i) for i in (2, 4, 6)])
        slots_self(s_send, s_recv, dr_sem, chunk).start()
        across_z = [slots_copy(s_send, s_recv, ds_sem, dr_sem, chunk, i) for i in (1, 3, 5, 7)]
        crossing.extend(across_z)

        @pl.when(far)
        def _():
            for copy in across_z:
                copy.start()

    with jax.named_scope("wait_x"):
        pltpu.make_async_copy(x_v, x_v, x_sem.at[0]).wait()

    def hidden(half, weights):
        def body(chunk, carry):
            rows = x_v[pl.ds(2 * chunk, 2)].reshape(128, 1024)
            both = jnp.dot(rows, weights[...].reshape(1024, 512), preferred_element_type=F32)
            gate, up = both[:, :256], both[:, 256:]
            sig = jax.nn.sigmoid(gate)
            act = gate * sig
            act_v[half, chunk] = act
            fac_v[half, chunk] = up * sig * (1.0 + gate * (1.0 - sig))
            hid_v[chunk, :, pl.ds(256 * half, 256)] = (act * up).astype(BF16)
            return carry

        lax.fori_loop(0, 2, body, 0)

    def d_terms(half, chunk, down):
        rows = s_recv[pl.ds(2 * chunk, 2)].reshape(128, 1024)
        dh = lax.dot_general(rows, down[...].reshape(256, 1024), NT, preferred_element_type=F32)
        d_both = jnp.concatenate(
            [(dh * fac_v[half, chunk]).astype(BF16), (dh * act_v[half, chunk]).astype(BF16)], axis=1
        )
        dg_v[half, chunk] = d_both

    def slot_grads(chunk):
        total = lax.dot_general(
            dg_v[0, chunk], wgu[...].reshape(1024, 512), NT, preferred_element_type=F32
        ) + lax.dot_general(dg_v[1, chunk], pgu[...].reshape(1024, 512), NT, preferred_element_type=F32)
        sg_v[pl.ds(2 * chunk, 2)] = total.astype(BF16).reshape(2, 64, 1024)

    def weight_terms(half, s):
        z = (zl + 1 + s) % 2

        def body(q, carry):
            cols = pl.ds(pl.multiple_of((2 * z + q) * 256, 256), 256)
            at = pl.ds(4 * q, 4)
            right = hid_v[:, :, pl.ds(256 * half, 256)].reshape(256, 256)
            out = lax.dot_general(s_recv[:, :, cols].reshape(256, 256), right, TN, preferred_element_type=F32)
            out = out.reshape(4, 2, 32, 256)
            rf[half, s, at, :, :, pl.ds(0, 256)] = out
            rb[half, s, at, :, :, pl.ds(0, 256)] = out.astype(BF16)
            right = dg_v[half].reshape(256, 512)
            out = lax.dot_general(x_v[:, :, cols].reshape(256, 256), right, TN, preferred_element_type=F32)
            out = out.reshape(4, 2, 32, 512)
            rf[half, s, at, :, :, pl.ds(256, 512)] = out
            rb[half, s, at, :, :, pl.ds(256, 512)] = out.astype(BF16)
            return carry

        lax.fori_loop(0, 2, body, 0)
        start([core_copy(half, s)])

    def core_copy(g, s):
        return remote(rb.at[g, s, :, 1 - core], drecv.at[g, s], cs_sem.at[0], cr_sem.at[g, s], (dp_core, mem))

    def term(g, s, owner):
        return rf[g, s, owner, core] + drecv[g, s, owner].astype(F32)

    def long_copy(g, s, t):
        at = (g, s, t)
        return remote(lsend.at[at], lrecv.at[at], cs_sem.at[1], lsr_sem.at[at], (dp_fwd, mem))

    def short_copy(g, s, t):
        at = (g, s, t)
        return remote(ssend.at[at], srecv.at[at], cs_sem.at[2], ssr_sem.at[at], (dp_bwd, mem))

    def ring_first(g, s):
        core_copy(g, s).wait_recv()
        lsend[g, s, 0] = term(g, s, (y + 4) % 8).astype(BF16)
        start([long_copy(g, s, 0)])
        ssend[g, s, 0] = term(g, s, (y - 3 * step + 8) % 8).astype(BF16)
        start([short_copy(g, s, 0)])

    def ring_next(g, s, t):
        own = term(g, s, (y + (4 - t) * step + 8) % 8)
        long_copy(g, s, t - 1).wait_recv()
        lsend[g, s, t] = (own + lrecv[g, s, t - 1].astype(F32)).astype(BF16)
        start([long_copy(g, s, t)])
        if t < 3:
            own = term(g, s, (y - (3 - t) * step + 8) % 8)
            short_copy(g, s, t - 1).wait_recv()
            ssend[g, s, t] = (own + srecv[g, s, t - 1].astype(F32)).astype(BF16)
            start([short_copy(g, s, t)])

    def z_copy(g, s):
        n = (0, None, 1, 2)[2 * g + s]
        dev = ((dp_z, dp)[s], (mem, partner)[g])
        return remote(finb.at[g, s], zd.at[n], cs_sem.at[3], zr_sem.at[n], dev)

    def ring_last(g, s):
        own = term(g, s, y)
        short_copy(g, s, 2).wait_recv()
        own = own + srecv[g, s, 2].astype(F32)
        long_copy(g, s, 3).wait_recv()
        own = own + lrecv[g, s, 3].astype(F32)
        if g == 0 and s == 1:
            fin[...] = own
        else:
            finb[g, s] = own.astype(BF16)
            start([z_copy(g, s)])

    def slots_arrive(chunk):
        slots_wait(s_recv, dr_sem, chunk)

    from_bwd = (y - step + 8) % 4
    from_fwd = (y + step + 8) % 4
    across = (y + 2) % 4

    def first_piece(h):
        weights_wait(0, h, quarter, core)
        relays = weights_copy(8, h, pgu, pd, quarter, core, (dp_z, mem), 0)

        @pl.when(near)
        def _():
            for copy in relays:
                copy.start()

        pass_on(1, h, quarter, (dp_fwd, mem))
        pass_on(2, h, quarter, (dp_bwd, mem))
        pass_on(4, h, quarter, (dp_core, mem))

    def second_piece(h):
        weights_wait(1, h, from_bwd, core)
        pass_on(3, h, from_bwd, (dp_fwd, mem))
        pass_on(5, h, from_bwd, (dp_core, mem))
        weights_wait(2, h, from_fwd, core)
        pass_on(6, h, from_fwd, (dp_core, mem))

    def third_piece(h):
        weights_wait(3, h, across, core)
        pass_on(7, h, across, (dp_core, mem))

    def last_piece(h):
        weights_wait(4, h, quarter, 1 - core)
        weights_wait(5, h, from_fwd, 1 - core)
        weights_wait(6, h, from_bwd, 1 - core)
        weights_wait(7, h, across, 1 - core)

    def tokens(chunk):
        slots_wait(ret_v, rr_sem, chunk)
        for mb in (2 * chunk, 2 * chunk + 1):
            gin_v[mb] = lax.dot_general(mix_v[mb], ret_v[mb], TN, preferred_element_type=F32).astype(BF16)

    with jax.named_scope("hidden0"):
        hidden(0, wgu)
    with jax.named_scope("w0a"):
        first_piece(0)
    with jax.named_scope("w0b"):
        first_piece(1)

    @pl.when(near)
    def _():
        for copy in crossing:
            copy.start()

    with jax.named_scope("w1a"):
        second_piece(0)
    with jax.named_scope("w1b"):
        second_piece(1)
    with jax.named_scope("slots0"):
        slots_arrive(0)
    with jax.named_scope("d_own0"):
        d_terms(0, 0, wd)
    with jax.named_scope("slots1"):
        slots_arrive(1)
    with jax.named_scope("d_own1"):
        d_terms(0, 1, wd)
    with jax.named_scope("weights0"):
        weight_terms(0, 0)
        weight_terms(0, 1)
    with jax.named_scope("w3"):
        third_piece(0)
        third_piece(1)
    with jax.named_scope("ring_first0"):
        ring_first(0, 0)
        ring_first(0, 1)
    with jax.named_scope("wlast"):
        last_piece(0)
        last_piece(1)
    with jax.named_scope("hidden1"):
        hidden(1, pgu)
    with jax.named_scope("d_partner"):
        d_terms(1, 0, pd)
        d_terms(1, 1, pd)
    with jax.named_scope("weights1"):
        weight_terms(1, 0)
        weight_terms(1, 1)
    with jax.named_scope("ring_next0_1"):
        ring_next(0, 0, 1)
        ring_next(0, 1, 1)
    with jax.named_scope("slot_grads0"):
        slot_grads(0)
        start([slots_copy(sg_v, ret_v, rs_sem, rr_sem, 0, i) for i in range(1, 8)])
        slots_self(sg_v, ret_v, rr_sem, 0).start()
    with jax.named_scope("ring_first1"):
        ring_first(1, 0)
        ring_first(1, 1)
    with jax.named_scope("slot_grads1"):
        slot_grads(1)
        start([slots_copy(sg_v, ret_v, rs_sem, rr_sem, 1, i) for i in range(1, 8)])
        slots_self(sg_v, ret_v, rr_sem, 1).start()
    with jax.named_scope("ring_next0_2"):
        ring_next(0, 0, 2)
        ring_next(0, 1, 2)
    with jax.named_scope("ring_next1_1"):
        ring_next(1, 0, 1)
        ring_next(1, 1, 1)
    with jax.named_scope("ring_next0_3"):
        ring_next(0, 0, 3)
        ring_next(0, 1, 3)
    with jax.named_scope("ring_next1_2"):
        ring_next(1, 0, 2)
        ring_next(1, 1, 2)
    with jax.named_scope("ring_last0"):
        ring_last(0, 0)
        ring_last(0, 1)
    with jax.named_scope("tokens0"):
        tokens(0)
    with jax.named_scope("ring_next1_3"):
        ring_next(1, 0, 3)
        ring_next(1, 1, 3)
    with jax.named_scope("tokens1"):
        tokens(1)
    with jax.named_scope("ring_last1"):
        ring_last(1, 0)
        ring_last(1, 1)

    with jax.named_scope("wait_z"):
        for copy in (z_copy(0, 0), z_copy(1, 0), z_copy(1, 1)):
            copy.wait_recv()
    total = fin[...]
    for n in range(3):
        total = total + zd[n].astype(F32)
    total = total * (1.0 / 128.0)
    down_v[...] = total[:, :256]
    gate_v[...] = total[:, 256:512]
    up_v[...] = total[:, 512:]

    def left(ref, sem):
        pltpu.make_async_copy(ref, ref, sem).wait()

    with jax.named_scope("wait_sends"):
        left(s_send.at[:, pl.ds(0, 56)], ds_sem.at[0])
        left(sg_v.at[:, pl.ds(0, 56)], rs_sem.at[0])
        left(pgu.at[:, :, :, pl.ds(0, 56)], ws_sem.at[0, 0])
        left(pd.at[:, :, :, :, pl.ds(0, 896)], ws_sem.at[0, 1])
        left(drecv, cs_sem.at[0])
        left(lsend, cs_sem.at[1])
        left(ssend, cs_sem.at[2])
        left(zd, cs_sem.at[3])

        @pl.when(near)
        def _():
            left(pgu.at[0, pl.ds(0, 2)], ws_sem.at[1, 0])
            left(pd.at[0, pl.ds(0, 2)], ws_sem.at[1, 1])


def per_device(grad_out, routes, route_probs, dispatched, w_gate, w_up, w_down):
    wg = w_gate.reshape(2, 4, 2, 64, 256)
    wu = w_up.reshape(2, 4, 2, 64, 256)
    wd = w_down.reshape(2, 4, 2, 16, 1024)
    hbm = pl.BlockSpec(memory_space=pltpu.HBM)
    vmem = pl.BlockSpec(memory_space=pltpu.VMEM)
    dma = pltpu.SemaphoreType.DMA
    V = pltpu.VMEM
    results = pl.pallas_call(
        kernel,
        out_shape=(V((4, 64, 1024), BF16),) + (V((32, 256), F32),) * 3,
        in_specs=[hbm] * 7,
        out_specs=(vmem,) * 4,
        scratch_shapes=[
            V((4, 8, 64), jnp.int32),
            V((4, 8, 64), BF16),
            V((4, 64, 1024), BF16),
            V((4, 64, 1024), BF16),
            V((2, 4, 2, 64, 512), BF16),
            V((2, 4, 2, 16, 1024), BF16),
            V((2, 4, 2, 64, 512), BF16),
            V((2, 4, 2, 16, 1024), BF16),
            V((4, 64, 64), BF16),
            V((4, 64, 1024), BF16),
            V((4, 64, 1024), BF16),
            V((2, 2, 128, 256), F32),
            V((2, 2, 128, 256), F32),
            V((2, 128, 512), BF16),
            V((2, 2, 128, 512), BF16),
            V((4, 64, 1024), BF16),
            V((4, 64, 1024), BF16),
            V((2, 2, 8, 2, 32, 768), F32),
            V((2, 2, 8, 2, 32, 768), BF16),
            V((2, 2, 8, 32, 768), BF16),
            V((2, 2, 4, 32, 768), BF16),
            V((2, 2, 4, 32, 768), BF16),
            V((2, 2, 3, 32, 768), BF16),
            V((2, 2, 3, 32, 768), BF16),
            V((32, 768), F32),
            V((2, 2, 32, 768), BF16),
            V((3, 32, 768), BF16),
            dma((6,)), dma((1,)),
            dma((1,)), dma((2,)), dma((1,)), dma((2,)),
            dma((2, 2)), dma((8, 2, 2)), dma((4,)), dma((2, 2)),
            dma((2, 2, 4)), dma((2, 2, 3)), dma((3,)),
        ],
        compiler_params=pltpu.CompilerParams(
            collective_id=0, has_side_effects=True, vmem_limit_bytes=48000000
        ),
        name="moe_backward",
    )(
        *(
            pltpu.with_memory_space_constraint(a, pltpu.HBM)
            for a in (
                grad_out, jnp.swapaxes(routes, 1, 2), jnp.swapaxes(route_probs, 1, 2), dispatched, wg, wu, wd
            )
        )
    )

    def store(a, b, c, d, out_a, out_b, out_c, out_d, sem):
        copies = [
            pltpu.make_async_copy(src, dst, sem.at[n])
            for n, (src, dst) in enumerate(((a, out_a), (b, out_b), (c, out_c), (d, out_d)))
        ]
        for copy in copies:
            copy.start()
        for copy in copies:
            copy.wait()

    return pl.pallas_call(
        store,
        out_shape=tuple(jax.ShapeDtypeStruct(r.shape, r.dtype) for r in results),
        in_specs=[vmem] * 4,
        out_specs=(hbm,) * 4,
        scratch_shapes=[dma((4,))],
        compiler_params=pltpu.CompilerParams(vmem_limit_bytes=1000000),
        name="store_results",
    )(*results)


def solution(mesh):
    return jax.shard_map(
        per_device,
        mesh=mesh,
        in_specs=(
            P(None, ("dp", "expert"), None),
            P(None, ("dp", "expert"), None),
            P(None, ("dp", "expert"), None),
            P(None, ("dp", "expert"), None),
            P(None, "expert"),
            P(None, "expert"),
            P("expert", None),
        ),
        out_specs=(
            P(None, ("dp", "expert"), None),
            P("dp", "expert"),
            P("dp", "expert"),
            P("dp", "expert"),
        ),
        check_vma=False,
    )
```

```python
import jax
import jax.numpy as jnp
from jax import lax
from jax.experimental import pallas as pl
from jax.experimental.pallas import tpu as pltpu
from jax.sharding import PartitionSpec as P

MESH = pl.DeviceIdType.MESH
F32 = jnp.float32
BF16 = jnp.bfloat16

NT = (((1,), (1,)), ((), ()))
TN = (((0,), (0,)), ((), ()))


def kernel(
    dy_hbm, routes_hbm, probs_hbm, disp_hbm, wg_hbm, wu_hbm, wd_hbm,
    gin_v, gate_v, up_v, down_v,
    routes_v, probs_v, dy_v, x_v, wgu, wd, pgu, pd,
    mix_v, s_send, s_recv, act_v, fac_v, hid_v, dg_v, sg_v, ret_v,
    rf, rb, drecv, lsend, lrecv, ssend, srecv, fin, finb, zd, zsend, zrecv,
    in_sem, x_sem,
    ds_sem, dr_sem, rs_sem, rr_sem,
    ws_sem, wr_sem, cs_sem, cr_sem,
    lsr_sem, ssr_sem, zr_sem,
):
    dp = lax.axis_index("dp")
    mem = lax.axis_index("expert")
    core = dp % 2
    y = (dp // 2) % 8
    zl = dp // 16
    step = 1 - 2 * core
    mine = mem // 2
    zh = mem % 4
    low = (zh * (3 - zh)) // 2

    def peer_of(e):
        return 4 * (e // 2) + low + (e % 2) * (3 - 2 * low)

    partner = mem + 1 - 2 * (mem % 2)
    dp_core = dp + 1 - 2 * core
    dp_fwd = zl * 16 + ((y + step + 8) % 8) * 2 + core
    dp_bwd = zl * 16 + ((y - step + 8) % 8) * 2 + core
    dp_z = (1 - zl) * 16 + y * 2 + core

    def remote(src, dst, ssem, rsem, dev):
        return pltpu.make_async_remote_copy(
            src_ref=src, dst_ref=dst, send_sem=ssem, recv_sem=rsem,
            device_id=dev, device_id_type=MESH,
        )

    barrier = pltpu.get_barrier_semaphore()
    peers = [(dp, peer_of((mine + i) % 8)) for i in range(1, 8)]
    peers += [(dp, partner), (dp_core, mem), (dp_fwd, mem), (dp_bwd, mem), (dp_z, mem), (dp_z, partner)]
    for dev in peers:
        pl.semaphore_signal(barrier, inc=1, device_id=dev, device_id_type=MESH)

    loads = [
        pltpu.make_async_copy(wg_hbm, wgu.at[:, :, :, :, pl.ds(0, 256)], in_sem.at[3]),
        pltpu.make_async_copy(wu_hbm, wgu.at[:, :, :, :, pl.ds(256, 256)], in_sem.at[4]),
        pltpu.make_async_copy(wd_hbm, wd, in_sem.at[5]),
        pltpu.make_async_copy(routes_hbm, routes_v, in_sem.at[0]),
        pltpu.make_async_copy(probs_hbm, probs_v, in_sem.at[1]),
        pltpu.make_async_copy(dy_hbm, dy_v, in_sem.at[2]),
    ]
    for load in loads:
        load.start()
    with jax.named_scope("barrier"):
        for load in loads[:3]:
            load.wait()
        pl.semaphore_wait(barrier, len(peers))

    quarter = y % 4

    def weights_copy(n, h, src_a, src_b, where, side, dev, come=None):
        come = n if come is None else come
        kind = 0 if 0 < n < 8 else 1
        return [
            remote(src_a.at[h, where, side], pgu.at[h, where, side], ws_sem.at[kind, 0], wr_sem.at[come, h, 0], dev),
            remote(src_b.at[h, where, side], pd.at[h, where, side], ws_sem.at[kind, 1], wr_sem.at[come, h, 1], dev),
        ]

    def start(copies):
        for copy in copies:
            copy.start()

    def weights_wait(n, h, where, side):
        for copy in weights_copy(n, h, pgu, pd, where, side, (dp_core, mem)):
            copy.wait_recv()

    def handle(n, h, where, onward):
        held = weights_copy(n, h, pgu, pd, where, core, (dp_core, mem))
        further = [weights_copy(to, h, pgu, pd, where, core, dev) for to, dev in onward]
        relay = weights_copy(8, h, pgu, pd, where, core, (dp_z, mem), 0) if n == 0 else ()
        for k in range(2):
            held[k].wait_recv()
            if n == 0:

                @pl.when(near)
                def _():
                    relay[k].start()

            for copies in further:
                copies[k].start()

    near = (zl + zh) % 2 == 1
    far = (zl + zh) % 2 == 0
    near_sends = []
    for h in range(2):
        near_sends += weights_copy(0, h, wgu, wd, quarter, core, (dp_z, partner))

    @pl.when(near)
    def _():
        for copy in near_sends:
            copy.start()

    with jax.named_scope("wait_in"):
        for load in loads[3:]:
            load.wait()

    def route(mb, carry):
        ids = routes_v[mb]
        probs = probs_v[mb].astype(F32)
        lane = lax.broadcasted_iota(jnp.int32, (64, 64), 1)
        row = lax.broadcasted_iota(jnp.int32, (64, 64), 0)
        expert = lax.shift_right_logical(row, 3)
        place = lax.bitwise_and(row, 7)
        hit = jnp.zeros((64, 64), F32)
        weight = jnp.zeros((64, 64), F32)
        for k in range(8):
            same = ids[k : k + 1, :] == expert
            hit = hit + jnp.where(same, 1.0, 0.0)
            weight = weight + jnp.where(same, probs[k : k + 1, :], 0.0)
        earlier = jnp.where(row < lane, 1.0, 0.0).astype(BF16)
        rank = jnp.dot(hit.astype(BF16), earlier, preferred_element_type=F32)
        chosen = jnp.where(rank == place.astype(F32), hit, 0.0)
        mix_v[mb] = chosen.astype(BF16)
        weighted = (chosen * weight).astype(BF16)
        scaled = jnp.dot(weighted, dy_v[mb], preferred_element_type=F32)
        s_send[mb] = scaled.astype(BF16)
        return carry

    x_loads = []
    for j in range(8):
        src = 4 * (j // 2) + (low if j % 2 == 0 else 3 - low)
        x_loads.append(
            pltpu.make_async_copy(
                disp_hbm.at[:, pl.ds(pl.multiple_of(src * 8, 8), 8)],
                x_v.at[:, pl.ds(j * 8, 8)],
                x_sem.at[0],
            )
        )
    for load in x_loads:
        load.start()
    def slots_copy(src, dst, sem_s, sem_r, chunk, i):
        to = (mine + i) % 8
        return remote(
            src.at[pl.ds(2 * chunk, 2), pl.ds(pl.multiple_of(to * 8, 8), 8)],
            dst.at[pl.ds(2 * chunk, 2), pl.ds(pl.multiple_of(mine * 8, 8), 8)],
            sem_s.at[0],
            sem_r.at[chunk],
            (dp, peer_of(to)),
        )

    def slots_self(src, dst, sem_r, chunk):
        at = pl.ds(pl.multiple_of(mine * 8, 8), 8)
        return pltpu.make_async_copy(
            src.at[pl.ds(2 * chunk, 2), at], dst.at[pl.ds(2 * chunk, 2), at], sem_r.at[chunk]
        )

    def slots_wait(dst, sem_r, chunk):
        rows = dst.at[pl.ds(2 * chunk, 2)]
        pltpu.make_async_copy(rows, rows, sem_r.at[chunk]).wait()

    crossing = []
    for chunk in range(2):
        with jax.named_scope("route"):
            lax.fori_loop(2 * chunk, 2 * chunk + 2, route, 0)
        start([slots_copy(s_send, s_recv, ds_sem, dr_sem, chunk, i) for i in (2, 4, 6)])
        slots_self(s_send, s_recv, dr_sem, chunk).start()
        across_z = [slots_copy(s_send, s_recv, ds_sem, dr_sem, chunk, i) for i in (1, 3, 5, 7)]
        crossing.extend(across_z)

        @pl.when(far)
        def _():
            for copy in across_z:
                copy.start()

    with jax.named_scope("wait_x"):
        pltpu.make_async_copy(x_v, x_v, x_sem.at[0]).wait()

    def hidden(half, weights):
        def body(chunk, carry):
            rows = x_v[pl.ds(2 * chunk, 2)].reshape(128, 1024)
            both = jnp.dot(rows, weights[...].reshape(1024, 512), preferred_element_type=F32)
            gate, up = both[:, :256], both[:, 256:]
            sig = jax.nn.sigmoid(gate)
            act = gate * sig
            act_v[half, chunk] = act
            fac_v[half, chunk] = up * sig * (1.0 + gate * (1.0 - sig))
            hid_v[chunk, :, pl.ds(256 * half, 256)] = (act * up).astype(BF16)
            return carry

        lax.fori_loop(0, 2, body, 0)

    def d_terms(half, chunk, down):
        rows = s_recv[pl.ds(2 * chunk, 2)].reshape(128, 1024)
        dh = lax.dot_general(rows, down[...].reshape(256, 1024), NT, preferred_element_type=F32)
        d_both = jnp.concatenate(
            [(dh * fac_v[half, chunk]).astype(BF16), (dh * act_v[half, chunk]).astype(BF16)], axis=1
        )
        dg_v[half, chunk] = d_both

    def slot_grads(chunk):
        total = lax.dot_general(
            dg_v[0, chunk], wgu[...].reshape(1024, 512), NT, preferred_element_type=F32
        ) + lax.dot_general(dg_v[1, chunk], pgu[...].reshape(1024, 512), NT, preferred_element_type=F32)
        sg_v[pl.ds(2 * chunk, 2)] = total.astype(BF16).reshape(2, 64, 1024)

    def weight_terms(half, s):
        z = (zl + 1 + s) % 2

        def body(q, carry):
            cols = pl.ds(pl.multiple_of((2 * z + q) * 256, 256), 256)
            at = pl.ds(4 * q, 4)
            right = hid_v[:, :, pl.ds(256 * half, 256)].reshape(256, 256)
            out = lax.dot_general(s_recv[:, :, cols].reshape(256, 256), right, TN, preferred_element_type=F32)
            out = out.reshape(4, 2, 32, 256)
            rf[half, s, at, :, :, pl.ds(0, 256)] = out
            rb[half, s, at, :, :, pl.ds(0, 256)] = out.astype(BF16)
            right = dg_v[half].reshape(256, 512)
            out = lax.dot_general(x_v[:, :, cols].reshape(256, 256), right, TN, preferred_element_type=F32)
            out = out.reshape(4, 2, 32, 512)
            rf[half, s, at, :, :, pl.ds(256, 512)] = out
            rb[half, s, at, :, :, pl.ds(256, 512)] = out.astype(BF16)
            return carry

        lax.fori_loop(0, 2, body, 0)
        start([core_copy(half, s)])

    is_far = (zl + zh + 1) % 2
    full = pl.ds(0, 768)
    downs = pl.ds(0, 256)
    gates = pl.ds(256, 512)
    streams = (
        (0, is_far, full),
        (0, 1 - is_far, downs),
        (1, 0, full),
        (1, 1, full),
        (0, 1, gates),
    )

    def core_copy(g, s):
        return remote(rb.at[g, s, :, 1 - core], drecv.at[g, s], cs_sem.at[0], cr_sem.at[g, s], (dp_core, mem))

    def term(n, owner):
        g, s, cols = streams[n]
        own = rf[g, s, owner, core, :, cols] + drecv[g, s, owner, :, cols].astype(F32)
        if n == 4:
            own = own + zrecv[owner].astype(F32)
        return own

    def at(ref, n, t):
        g, s, cols = streams[n]
        return ref.at[2 * g + s, t, :, cols]

    group = (1, 2, 3, 3, 4)

    def long_copy(n, t):
        return remote(at(lsend, n, t), at(lrecv, n, t), cs_sem.at[group[n]], lsr_sem.at[n, t], (dp_fwd, mem))

    def short_copy(n, t):
        return remote(at(ssend, n, t), at(srecv, n, t), cs_sem.at[group[n] + 4], ssr_sem.at[n, t], (dp_bwd, mem))

    def ring_first(n):
        at(lsend, n, 0)[...] = term(n, (y + 4) % 8).astype(BF16)
        start([long_copy(n, 0)])
        at(ssend, n, 0)[...] = term(n, (y - 3 * step + 8) % 8).astype(BF16)
        start([short_copy(n, 0)])

    def ring_next(n, t):
        own = term(n, (y + (4 - t) * step + 8) % 8)
        long_copy(n, t - 1).wait_recv()
        at(lsend, n, t)[...] = (own + at(lrecv, n, t - 1)[...].astype(F32)).astype(BF16)
        start([long_copy(n, t)])
        if t < 3:
            own = term(n, (y - (3 - t) * step + 8) % 8)
            short_copy(n, t - 1).wait_recv()
            at(ssend, n, t)[...] = (own + at(srecv, n, t - 1)[...].astype(F32)).astype(BF16)
            start([short_copy(n, t)])

    def ring_total(n):
        own = term(n, y)
        short_copy(n, 2).wait_recv()
        own = own + at(srecv, n, 2)[...].astype(F32)
        long_copy(n, 3).wait_recv()
        return own + at(lrecv, n, 3)[...].astype(F32)

    def partner_copy(s):
        return remote(finb.at[1 + s], zd.at[1 + s], cs_sem.at[9], zr_sem.at[1 + s], ((dp_z, dp)[s], partner))

    def other_z_copy(cols):
        return remote(finb.at[0, :, cols], zd.at[0, :, cols], cs_sem.at[10], zr_sem.at[0], (dp_z, mem))

    def z_first():
        return remote(zsend, zrecv, cs_sem.at[11], zr_sem.at[3], (dp_z, mem))

    def ring_last(n):
        if n in (2, 3):
            finb[n - 1] = ring_total(n).astype(BF16)
            start([partner_copy(n - 2)])
        elif n == 4:
            fin[:, gates] = ring_total(n)
        else:
            own = ring_total(n)
            cols = streams[n][2]
            sends_on, keeps = (near, far) if n == 0 else (far, near)

            @pl.when(sends_on)
            def _():
                finb[0, :, cols] = own.astype(BF16)
                other_z_copy(cols).start()

            @pl.when(keeps)
            def _():
                fin[:, cols] = own

    def slots_arrive(chunk):
        slots_wait(s_recv, dr_sem, chunk)

    from_bwd = (y - step + 8) % 4
    from_fwd = (y + step + 8) % 4
    across = (y + 2) % 4

    def first_piece(h):
        handle(0, h, quarter, ((1, (dp_fwd, mem)), (2, (dp_bwd, mem)), (4, (dp_core, mem))))

    def second_piece(h):
        handle(1, h, from_bwd, ((3, (dp_fwd, mem)), (5, (dp_core, mem))))
        handle(2, h, from_fwd, ((6, (dp_core, mem)),))

    def third_piece(h):
        handle(3, h, across, ((7, (dp_core, mem)),))

    def last_piece(h):
        weights_wait(4, h, quarter, 1 - core)
        weights_wait(5, h, from_fwd, 1 - core)
        weights_wait(6, h, from_bwd, 1 - core)
        weights_wait(7, h, across, 1 - core)

    def tokens(chunk):
        slots_wait(ret_v, rr_sem, chunk)
        for mb in (2 * chunk, 2 * chunk + 1):
            gin_v[mb] = lax.dot_general(mix_v[mb], ret_v[mb], TN, preferred_element_type=F32).astype(BF16)

    with jax.named_scope("hidden0"):
        hidden(0, wgu)
    with jax.named_scope("w0a"):
        first_piece(0)
    with jax.named_scope("w0b"):
        first_piece(1)

    @pl.when(near)
    def _():
        for copy in crossing:
            copy.start()

    with jax.named_scope("w1a"):
        second_piece(0)
    with jax.named_scope("w1b"):
        second_piece(1)
    with jax.named_scope("slots0"):
        slots_arrive(0)
    with jax.named_scope("d_own0"):
        d_terms(0, 0, wd)
    with jax.named_scope("slots1"):
        slots_arrive(1)
    with jax.named_scope("d_own1"):
        d_terms(0, 1, wd)
    with jax.named_scope("weights0"):
        weight_terms(0, 0)
        weight_terms(0, 1)
    with jax.named_scope("w3"):
        third_piece(0)
        third_piece(1)
    with jax.named_scope("wlast"):
        last_piece(0)
        last_piece(1)
    with jax.named_scope("hidden1"):
        hidden(1, pgu)
    with jax.named_scope("ring_first0"):
        core_copy(0, 0).wait_recv()
        core_copy(0, 1).wait_recv()
        ring_first(0)

    @pl.when(far)
    def _():
        zsend[...] = (rf[0, 0, :, core, :, gates] + drecv[0, 0, :, :, gates].astype(F32)).astype(BF16)
        z_first().start()

    with jax.named_scope("ring_first0b"):
        ring_first(1)
    with jax.named_scope("d_partner"):
        d_terms(1, 0, pd)
        d_terms(1, 1, pd)
    with jax.named_scope("weights1"):
        weight_terms(1, 0)
        weight_terms(1, 1)
    with jax.named_scope("ring_next0_1"):
        ring_next(0, 1)
        ring_next(1, 1)
    with jax.named_scope("slot_grads0"):
        slot_grads(0)
        start([slots_copy(sg_v, ret_v, rs_sem, rr_sem, 0, i) for i in range(1, 8)])
        slots_self(sg_v, ret_v, rr_sem, 0).start()
    with jax.named_scope("ring_first1"):
        for s in range(2):
            core_copy(1, s).wait_recv()
            ring_first(2 + s)
    with jax.named_scope("slot_grads1"):
        slot_grads(1)
        start([slots_copy(sg_v, ret_v, rs_sem, rr_sem, 1, i) for i in range(1, 8)])
        slots_self(sg_v, ret_v, rr_sem, 1).start()
    with jax.named_scope("ring_next0_2"):
        ring_next(0, 2)
        ring_next(1, 2)
    with jax.named_scope("ring_next1_1"):
        ring_next(2, 1)
        ring_next(3, 1)
    with jax.named_scope("ring_next0_3"):
        ring_next(0, 3)
        ring_next(1, 3)
    with jax.named_scope("ring_next1_2"):
        ring_next(2, 2)
        ring_next(3, 2)
    with jax.named_scope("ring_last0"):
        ring_last(0)
        ring_last(1)

    @pl.when(near)
    def _():
        z_first().wait_recv()
        ring_first(4)

    with jax.named_scope("ring_next1_3"):
        ring_next(2, 3)
        ring_next(3, 3)

    @pl.when(near)
    def _():
        ring_next(4, 1)

    with jax.named_scope("ring_last1"):
        ring_last(2)
        ring_last(3)
    with jax.named_scope("tokens0"):
        tokens(0)

    @pl.when(near)
    def _():
        ring_next(4, 2)


    with jax.named_scope("late"):

        @pl.when(near)
        def _():
            ring_next(4, 3)
            ring_last(4)
            zd[0, :, gates] = jnp.zeros((32, 512), BF16)
            other_z_copy(downs).wait_recv()

        @pl.when(far)
        def _():
            other_z_copy(full).wait_recv()

    with jax.named_scope("tokens1"):
        tokens(1)
    with jax.named_scope("wait_z"):
        partner_copy(0).wait_recv()
        partner_copy(1).wait_recv()
    total = fin[...]
    for n in range(3):
        total = total + zd[n].astype(F32)
    total = total * (1.0 / 128.0)
    down_v[...] = total[:, :256]
    gate_v[...] = total[:, 256:512]
    up_v[...] = total[:, 512:]

    def left(ref, sem):
        pltpu.make_async_copy(ref, ref, sem).wait()

    with jax.named_scope("wait_sends"):
        left(s_send.at[:, pl.ds(0, 56)], ds_sem.at[0])
        left(sg_v.at[:, pl.ds(0, 56)], rs_sem.at[0])
        left(pgu.at[:, :, :, pl.ds(0, 56)], ws_sem.at[0, 0])
        left(pd.at[:, :, :, :, pl.ds(0, 896)], ws_sem.at[0, 1])
        left(drecv, cs_sem.at[0])
        left(lsend.at[is_far], cs_sem.at[1])
        left(ssend.at[is_far], cs_sem.at[5])
        left(lsend.at[1 - is_far, :, :, downs], cs_sem.at[2])
        left(ssend.at[1 - is_far, :, :, downs], cs_sem.at[6])
        left(lsend.at[pl.ds(2, 2)], cs_sem.at[3])
        left(ssend.at[pl.ds(2, 2)], cs_sem.at[7])
        left(finb.at[pl.ds(1, 2)], cs_sem.at[9])

        @pl.when(near)
        def _():
            left(pgu.at[0, pl.ds(0, 2)], ws_sem.at[1, 0])
            left(pd.at[0, pl.ds(0, 2)], ws_sem.at[1, 1])
            left(lsend.at[1, :, :, gates], cs_sem.at[4])
            left(ssend.at[1, :, :, gates], cs_sem.at[8])
            left(finb.at[0], cs_sem.at[10])

        @pl.when(far)
        def _():
            left(finb.at[0, :, downs], cs_sem.at[10])
            left(zsend, cs_sem.at[11])


def per_device(grad_out, routes, route_probs, dispatched, w_gate, w_up, w_down):
    wg = w_gate.reshape(2, 4, 2, 64, 256)
    wu = w_up.reshape(2, 4, 2, 64, 256)
    wd = w_down.reshape(2, 4, 2, 16, 1024)
    hbm = pl.BlockSpec(memory_space=pltpu.HBM)
    vmem = pl.BlockSpec(memory_space=pltpu.VMEM)
    dma = pltpu.SemaphoreType.DMA
    V = pltpu.VMEM
    results = pl.pallas_call(
        kernel,
        out_shape=(V((4, 64, 1024), BF16),) + (V((32, 256), F32),) * 3,
        in_specs=[hbm] * 7,
        out_specs=(vmem,) * 4,
        scratch_shapes=[
            V((4, 8, 64), jnp.int32),
            V((4, 8, 64), BF16),
            V((4, 64, 1024), BF16),
            V((4, 64, 1024), BF16),
            V((2, 4, 2, 64, 512), BF16),
            V((2, 4, 2, 16, 1024), BF16),
            V((2, 4, 2, 64, 512), BF16),
            V((2, 4, 2, 16, 1024), BF16),
            V((4, 64, 64), BF16),
            V((4, 64, 1024), BF16),
            V((4, 64, 1024), BF16),
            V((2, 2, 128, 256), F32),
            V((2, 2, 128, 256), F32),
            V((2, 128, 512), BF16),
            V((2, 2, 128, 512), BF16),
            V((4, 64, 1024), BF16),
            V((4, 64, 1024), BF16),
            V((2, 2, 8, 2, 32, 768), F32),
            V((2, 2, 8, 2, 32, 768), BF16),
            V((2, 2, 8, 32, 768), BF16),
            V((4, 4, 32, 768), BF16),
            V((4, 4, 32, 768), BF16),
            V((4, 3, 32, 768), BF16),
            V((4, 3, 32, 768), BF16),
            V((32, 768), F32),
            V((3, 32, 768), BF16),
            V((3, 32, 768), BF16),
            V((8, 32, 512), BF16),
            V((8, 32, 512), BF16),
            dma((6,)), dma((1,)),
            dma((1,)), dma((2,)), dma((1,)), dma((2,)),
            dma((2, 2)), dma((8, 2, 2)), dma((12,)), dma((2, 2)),
            dma((5, 4)), dma((5, 3)), dma((4,)),
        ],
        compiler_params=pltpu.CompilerParams(
            collective_id=0, has_side_effects=True, vmem_limit_bytes=48000000
        ),
        name="moe_backward",
    )(
        *(
            pltpu.with_memory_space_constraint(a, pltpu.HBM)
            for a in (
                grad_out, jnp.swapaxes(routes, 1, 2), jnp.swapaxes(route_probs, 1, 2), dispatched, wg, wu, wd
            )
        )
    )

    def store(a, b, c, d, out_a, out_b, out_c, out_d, sem):
        copies = [
            pltpu.make_async_copy(src, dst, sem.at[n])
            for n, (src, dst) in enumerate(((a, out_a), (b, out_b), (c, out_c), (d, out_d)))
        ]
        for copy in copies:
            copy.start()
        for copy in copies:
            copy.wait()

    return pl.pallas_call(
        store,
        out_shape=tuple(jax.ShapeDtypeStruct(r.shape, r.dtype) for r in results),
        in_specs=[vmem] * 4,
        out_specs=(hbm,) * 4,
        scratch_shapes=[dma((4,))],
        compiler_params=pltpu.CompilerParams(vmem_limit_bytes=1000000),
        name="store_results",
    )(*results)


def solution(mesh):
    return jax.shard_map(
        per_device,
        mesh=mesh,
        in_specs=(
            P(None, ("dp", "expert"), None),
            P(None, ("dp", "expert"), None),
            P(None, ("dp", "expert"), None),
            P(None, ("dp", "expert"), None),
            P(None, "expert"),
            P(None, "expert"),
            P("expert", None),
        ),
        out_specs=(
            P(None, ("dp", "expert"), None),
            P("dp", "expert"),
            P("dp", "expert"),
            P("dp", "expert"),
        ),
        check_vma=False,
    )
```

```python
import jax
import jax.numpy as jnp
from jax import lax
from jax.experimental import pallas as pl
from jax.experimental.pallas import tpu as pltpu
from jax.sharding import PartitionSpec as P

MESH = pl.DeviceIdType.MESH
F32 = jnp.float32
BF16 = jnp.bfloat16

NT = (((1,), (1,)), ((), ()))
TN = (((0,), (0,)), ((), ()))


def kernel(
    dy_hbm, routes_hbm, probs_hbm, disp_hbm, wg_hbm, wu_hbm, wd_hbm,
    gin_v, gate_v, up_v, down_v,
    routes_v, probs_v, dy_v, x_v, wgu, wd, pgu, pd,
    mix_v, s_send, s_recv, act_v, fac_v, hid_v, dg_v, sg_v, ret_v,
    rf, rb, drecv, lsend, lrecv, ssend, srecv, fin, finb, zd, zsend, zrecv,
    in_sem, x_sem,
    ds_sem, dr_sem, rs_sem, rr_sem,
    ws_sem, wr_sem, cs_sem, cr_sem,
    lsr_sem, ssr_sem, zr_sem,
):
    dp = lax.axis_index("dp")
    mem = lax.axis_index("expert")
    core = dp % 2
    y = (dp // 2) % 8
    zl = dp // 16
    step = 1 - 2 * core
    mine = mem // 2
    zh = mem % 4
    low = (zh * (3 - zh)) // 2

    def peer_of(e):
        return 4 * (e // 2) + low + (e % 2) * (3 - 2 * low)

    partner = mem + 1 - 2 * (mem % 2)
    dp_core = dp + 1 - 2 * core
    dp_fwd = zl * 16 + ((y + step + 8) % 8) * 2 + core
    dp_bwd = zl * 16 + ((y - step + 8) % 8) * 2 + core
    dp_z = (1 - zl) * 16 + y * 2 + core

    def remote(src, dst, ssem, rsem, dev):
        return pltpu.make_async_remote_copy(
            src_ref=src, dst_ref=dst, send_sem=ssem, recv_sem=rsem,
            device_id=dev, device_id_type=MESH,
        )

    barrier = pltpu.get_barrier_semaphore()
    peers = [(dp, peer_of((mine + i) % 8)) for i in range(1, 8)]
    peers += [(dp, partner), (dp_core, mem), (dp_fwd, mem), (dp_bwd, mem), (dp_z, mem), (dp_z, partner)]
    for dev in peers:
        pl.semaphore_signal(barrier, inc=1, device_id=dev, device_id_type=MESH)

    loads = [
        pltpu.make_async_copy(wg_hbm, wgu.at[:, :, :, :, pl.ds(0, 256)], in_sem.at[3]),
        pltpu.make_async_copy(wu_hbm, wgu.at[:, :, :, :, pl.ds(256, 256)], in_sem.at[4]),
        pltpu.make_async_copy(wd_hbm, wd, in_sem.at[5]),
        pltpu.make_async_copy(routes_hbm, routes_v, in_sem.at[0]),
        pltpu.make_async_copy(probs_hbm, probs_v, in_sem.at[1]),
        pltpu.make_async_copy(dy_hbm, dy_v, in_sem.at[2]),
    ]
    for load in loads:
        load.start()
    with jax.named_scope("barrier"):
        for load in loads[:3]:
            load.wait()
        pl.semaphore_wait(barrier, len(peers))

    quarter = y % 4

    def weights_copy(n, h, src_a, src_b, where, side, dev, come=None):
        come = n if come is None else come
        kind = 0 if 0 < n < 8 else 1
        return [
            remote(src_a.at[h, where, side], pgu.at[h, where, side], ws_sem.at[kind, 0], wr_sem.at[come, h, 0], dev),
            remote(src_b.at[h, where, side], pd.at[h, where, side], ws_sem.at[kind, 1], wr_sem.at[come, h, 1], dev),
        ]

    def start(copies):
        for copy in copies:
            copy.start()

    def weights_wait(n, h, where, side):
        for copy in weights_copy(n, h, pgu, pd, where, side, (dp_core, mem)):
            copy.wait_recv()

    def handle(n, h, where, onward):
        held = weights_copy(n, h, pgu, pd, where, core, (dp_core, mem))
        further = [weights_copy(to, h, pgu, pd, where, core, dev) for to, dev in onward]
        relay = weights_copy(8, h, pgu, pd, where, core, (dp_z, mem), 0) if n == 0 else ()
        for k in range(2):
            held[k].wait_recv()
            if n == 0:

                @pl.when(near)
                def _():
                    relay[k].start()

            for copies in further:
                copies[k].start()

    near = (zl + zh) % 2 == 1
    far = (zl + zh) % 2 == 0
    near_sends = []
    for h in range(2):
        near_sends += weights_copy(0, h, wgu, wd, quarter, core, (dp_z, partner))

    @pl.when(near)
    def _():
        for copy in near_sends:
            copy.start()

    with jax.named_scope("wait_in"):
        for load in loads[3:]:
            load.wait()

    def route(mb, carry):
        ids = routes_v[mb]
        probs = probs_v[mb].astype(F32)
        lane = lax.broadcasted_iota(jnp.int32, (64, 64), 1)
        row = lax.broadcasted_iota(jnp.int32, (64, 64), 0)
        expert = lax.shift_right_logical(row, 3)
        place = lax.bitwise_and(row, 7)
        hit = jnp.zeros((64, 64), F32)
        weight = jnp.zeros((64, 64), F32)
        for k in range(8):
            same = ids[k : k + 1, :] == expert
            hit = hit + jnp.where(same, 1.0, 0.0)
            weight = weight + jnp.where(same, probs[k : k + 1, :], 0.0)
        earlier = jnp.where(row < lane, 1.0, 0.0).astype(BF16)
        rank = jnp.dot(hit.astype(BF16), earlier, preferred_element_type=F32)
        chosen = jnp.where(rank == place.astype(F32), hit, 0.0)
        mix_v[mb] = chosen.astype(BF16)
        weighted = (chosen * weight).astype(BF16)
        scaled = jnp.dot(weighted, dy_v[mb], preferred_element_type=F32)
        s_send[mb] = scaled.astype(BF16)
        return carry

    x_loads = []
    for j in range(8):
        src = 4 * (j // 2) + (low if j % 2 == 0 else 3 - low)
        x_loads.append(
            pltpu.make_async_copy(
                disp_hbm.at[:, pl.ds(pl.multiple_of(src * 8, 8), 8)],
                x_v.at[:, pl.ds(j * 8, 8)],
                x_sem.at[0],
            )
        )
    for load in x_loads:
        load.start()
    def slots_copy(src, dst, sem_s, sem_r, chunk, i):
        to = (mine + i) % 8
        return remote(
            src.at[pl.ds(2 * chunk, 2), pl.ds(pl.multiple_of(to * 8, 8), 8)],
            dst.at[pl.ds(2 * chunk, 2), pl.ds(pl.multiple_of(mine * 8, 8), 8)],
            sem_s.at[0],
            sem_r.at[chunk],
            (dp, peer_of(to)),
        )

    def slots_self(src, dst, sem_r, chunk):
        at = pl.ds(pl.multiple_of(mine * 8, 8), 8)
        return pltpu.make_async_copy(
            src.at[pl.ds(2 * chunk, 2), at], dst.at[pl.ds(2 * chunk, 2), at], sem_r.at[chunk]
        )

    def slots_wait(dst, sem_r, chunk):
        rows = dst.at[pl.ds(2 * chunk, 2)]
        pltpu.make_async_copy(rows, rows, sem_r.at[chunk]).wait()

    crossing = []
    for chunk in range(2):
        with jax.named_scope("route"):
            lax.fori_loop(2 * chunk, 2 * chunk + 2, route, 0)
        start([slots_copy(s_send, s_recv, ds_sem, dr_sem, chunk, i) for i in (2, 4, 6)])
        slots_self(s_send, s_recv, dr_sem, chunk).start()
        across_z = [slots_copy(s_send, s_recv, ds_sem, dr_sem, chunk, i) for i in (1, 3, 5, 7)]
        crossing.extend(across_z)

        @pl.when(far)
        def _():
            for copy in across_z:
                copy.start()

    with jax.named_scope("wait_x"):
        pltpu.make_async_copy(x_v, x_v, x_sem.at[0]).wait()

    def hidden(half, weights):
        def body(chunk, carry):
            rows = x_v[pl.ds(2 * chunk, 2)].reshape(128, 1024)
            both = jnp.dot(rows, weights[...].reshape(1024, 512), preferred_element_type=F32)
            gate, up = both[:, :256], both[:, 256:]
            sig = jax.nn.sigmoid(gate)
            act = gate * sig
            act_v[half, chunk] = act
            fac_v[half, chunk] = up * sig * (1.0 + gate * (1.0 - sig))
            hid_v[chunk, :, pl.ds(256 * half, 256)] = (act * up).astype(BF16)
            return carry

        lax.fori_loop(0, 2, body, 0)

    def d_terms(half, chunk, down):
        rows = s_recv[pl.ds(2 * chunk, 2)].reshape(128, 1024)
        dh = lax.dot_general(rows, down[...].reshape(256, 1024), NT, preferred_element_type=F32)
        d_both = jnp.concatenate(
            [(dh * fac_v[half, chunk]).astype(BF16), (dh * act_v[half, chunk]).astype(BF16)], axis=1
        )
        dg_v[half, chunk] = d_both

    def slot_grads(chunk):
        total = lax.dot_general(
            dg_v[0, chunk], wgu[...].reshape(1024, 512), NT, preferred_element_type=F32
        ) + lax.dot_general(dg_v[1, chunk], pgu[...].reshape(1024, 512), NT, preferred_element_type=F32)
        sg_v[pl.ds(2 * chunk, 2)] = total.astype(BF16).reshape(2, 64, 1024)

    def weight_terms(half, s):
        z = (zl + 1 + s) % 2

        def body(q, carry):
            cols = pl.ds(pl.multiple_of((2 * z + q) * 256, 256), 256)
            at = pl.ds(4 * q, 4)
            right = hid_v[:, :, pl.ds(256 * half, 256)].reshape(256, 256)
            out = lax.dot_general(s_recv[:, :, cols].reshape(256, 256), right, TN, preferred_element_type=F32)
            out = out.reshape(4, 2, 32, 256)
            rf[half, s, at, :, :, pl.ds(0, 256)] = out
            rb[half, s, at, :, :, pl.ds(0, 256)] = out.astype(BF16)
            right = dg_v[half].reshape(256, 512)
            out = lax.dot_general(x_v[:, :, cols].reshape(256, 256), right, TN, preferred_element_type=F32)
            out = out.reshape(4, 2, 32, 512)
            rf[half, s, at, :, :, pl.ds(256, 512)] = out
            rb[half, s, at, :, :, pl.ds(256, 512)] = out.astype(BF16)
            return carry

        lax.fori_loop(0, 2, body, 0)
        start([core_copy(half, s)])

    is_far = (zl + zh + 1) % 2
    full = pl.ds(0, 768)
    downs = pl.ds(0, 256)
    gates = pl.ds(256, 512)
    streams = (
        (0, is_far, full),
        (0, 1 - is_far, downs),
        (1, 0, full),
        (1, 1, full),
        (0, 1, gates),
    )

    def core_copy(g, s):
        return remote(rb.at[g, s, :, 1 - core], drecv.at[g, s], cs_sem.at[0], cr_sem.at[g, s], (dp_core, mem))

    def term(n, owner):
        g, s, cols = streams[n]
        own = rf[g, s, owner, core, :, cols] + drecv[g, s, owner, :, cols].astype(F32)
        if n == 4:
            own = own + zrecv[owner].astype(F32)
        return own

    def at(ref, n, t):
        g, s, cols = streams[n]
        return ref.at[2 * g + s, t, :, cols]

    group = (1, 2, 3, 3, 4)

    def long_copy(n, t):
        return remote(at(lsend, n, t), at(lrecv, n, t), cs_sem.at[group[n]], lsr_sem.at[n, t], (dp_fwd, mem))

    def short_copy(n, t):
        return remote(at(ssend, n, t), at(srecv, n, t), cs_sem.at[group[n] + 4], ssr_sem.at[n, t], (dp_bwd, mem))

    def ring_first(n):
        at(lsend, n, 0)[...] = term(n, (y + 4) % 8).astype(BF16)
        start([long_copy(n, 0)])
        at(ssend, n, 0)[...] = term(n, (y - 3 * step + 8) % 8).astype(BF16)
        start([short_copy(n, 0)])

    def ring_next(n, t):
        own = term(n, (y + (4 - t) * step + 8) % 8)
        long_copy(n, t - 1).wait_recv()
        at(lsend, n, t)[...] = (own + at(lrecv, n, t - 1)[...].astype(F32)).astype(BF16)
        start([long_copy(n, t)])
        if t < 3:
            own = term(n, (y - (3 - t) * step + 8) % 8)
            short_copy(n, t - 1).wait_recv()
            at(ssend, n, t)[...] = (own + at(srecv, n, t - 1)[...].astype(F32)).astype(BF16)
            start([short_copy(n, t)])

    def ring_total(n):
        own = term(n, y)
        short_copy(n, 2).wait_recv()
        own = own + at(srecv, n, 2)[...].astype(F32)
        long_copy(n, 3).wait_recv()
        return own + at(lrecv, n, 3)[...].astype(F32)

    def partner_copy(s):
        return remote(finb.at[1 + s], zd.at[1 + s], cs_sem.at[9], zr_sem.at[1 + s], ((dp_z, dp)[s], partner))

    def other_z_copy(cols):
        return remote(finb.at[0, :, cols], zd.at[0, :, cols], cs_sem.at[10], zr_sem.at[0], (dp_z, mem))

    def z_first():
        return remote(zsend, zrecv, cs_sem.at[11], zr_sem.at[3], (dp_z, mem))

    def ring_last(n):
        if n in (2, 3):
            finb[n - 1] = ring_total(n).astype(BF16)
            start([partner_copy(n - 2)])
        elif n == 4:
            fin[:, gates] = ring_total(n)
        else:
            own = ring_total(n)
            cols = streams[n][2]
            sends_on, keeps = (near, far) if n == 0 else (far, near)

            @pl.when(sends_on)
            def _():
                finb[0, :, cols] = own.astype(BF16)
                other_z_copy(cols).start()

            @pl.when(keeps)
            def _():
                fin[:, cols] = own

    def slots_arrive(chunk):
        slots_wait(s_recv, dr_sem, chunk)

    from_bwd = (y - step + 8) % 4
    from_fwd = (y + step + 8) % 4
    across = (y + 2) % 4

    def first_piece(h):
        handle(0, h, quarter, ((1, (dp_fwd, mem)), (2, (dp_bwd, mem)), (4, (dp_core, mem))))

    def second_piece(h):
        handle(1, h, from_bwd, ((3, (dp_fwd, mem)), (5, (dp_core, mem))))
        handle(2, h, from_fwd, ((6, (dp_core, mem)),))

    def third_piece(h):
        handle(3, h, across, ((7, (dp_core, mem)),))

    def last_piece(h):
        weights_wait(4, h, quarter, 1 - core)
        weights_wait(5, h, from_fwd, 1 - core)
        weights_wait(6, h, from_bwd, 1 - core)
        weights_wait(7, h, across, 1 - core)

    def tokens(chunk):
        slots_wait(ret_v, rr_sem, chunk)
        for mb in (2 * chunk, 2 * chunk + 1):
            gin_v[mb] = lax.dot_general(mix_v[mb], ret_v[mb], TN, preferred_element_type=F32).astype(BF16)

    with jax.named_scope("hidden0"):
        hidden(0, wgu)
    with jax.named_scope("w0a"):
        first_piece(0)
    with jax.named_scope("w0b"):
        first_piece(1)

    @pl.when(near)
    def _():
        for copy in crossing:
            copy.start()

    with jax.named_scope("w1a"):
        second_piece(0)
    with jax.named_scope("w1b"):
        second_piece(1)
    with jax.named_scope("slots0"):
        slots_arrive(0)
    with jax.named_scope("d_own0"):
        d_terms(0, 0, wd)
    with jax.named_scope("slots1"):
        slots_arrive(1)
    with jax.named_scope("d_own1"):
        d_terms(0, 1, wd)
    with jax.named_scope("weights0"):
        weight_terms(0, 0)
        weight_terms(0, 1)
    with jax.named_scope("w3"):
        third_piece(0)
        third_piece(1)
    with jax.named_scope("wlast"):
        last_piece(0)
        last_piece(1)
    with jax.named_scope("hidden1"):
        hidden(1, pgu)
    with jax.named_scope("ring_first0"):
        core_copy(0, 0).wait_recv()
        core_copy(0, 1).wait_recv()
        ring_first(0)

    @pl.when(far)
    def _():
        zsend[...] = (rf[0, 0, :, core, :, gates] + drecv[0, 0, :, :, gates].astype(F32)).astype(BF16)
        z_first().start()

    with jax.named_scope("ring_first0b"):
        ring_first(1)
    with jax.named_scope("d_partner"):
        d_terms(1, 0, pd)
        d_terms(1, 1, pd)
    with jax.named_scope("weights1"):
        weight_terms(1, 0)
        weight_terms(1, 1)
    with jax.named_scope("slot_grads0"):
        slot_grads(0)
        start([slots_copy(sg_v, ret_v, rs_sem, rr_sem, 0, i) for i in range(1, 8)])
        slots_self(sg_v, ret_v, rr_sem, 0).start()
    with jax.named_scope("ring_next0_1"):
        ring_next(0, 1)
        ring_next(1, 1)
    with jax.named_scope("ring_first1"):
        for s in range(2):
            core_copy(1, s).wait_recv()
            ring_first(2 + s)
    with jax.named_scope("slot_grads1"):
        slot_grads(1)
        start([slots_copy(sg_v, ret_v, rs_sem, rr_sem, 1, i) for i in range(1, 8)])
        slots_self(sg_v, ret_v, rr_sem, 1).start()
    with jax.named_scope("ring_next0_2"):
        ring_next(0, 2)
        ring_next(1, 2)
    with jax.named_scope("ring_next1_1"):
        ring_next(2, 1)
        ring_next(3, 1)
    with jax.named_scope("ring_next0_3"):
        ring_next(0, 3)
        ring_next(1, 3)
    with jax.named_scope("ring_next1_2"):
        ring_next(2, 2)
        ring_next(3, 2)
    with jax.named_scope("ring_last0"):
        ring_last(0)
        ring_last(1)

    @pl.when(near)
    def _():
        z_first().wait_recv()
        ring_first(4)

    with jax.named_scope("ring_next1_3"):
        ring_next(2, 3)
        ring_next(3, 3)

    @pl.when(near)
    def _():
        ring_next(4, 1)

    with jax.named_scope("ring_last1"):
        ring_last(2)
        ring_last(3)
    with jax.named_scope("tokens0"):
        tokens(0)

    @pl.when(near)
    def _():
        ring_next(4, 2)


    with jax.named_scope("late"):

        @pl.when(near)
        def _():
            ring_next(4, 3)
            ring_last(4)
            zd[0, :, gates] = jnp.zeros((32, 512), BF16)
            other_z_copy(downs).wait_recv()

        @pl.when(far)
        def _():
            other_z_copy(full).wait_recv()

    with jax.named_scope("tokens1"):
        tokens(1)
    with jax.named_scope("wait_z"):
        partner_copy(0).wait_recv()
        partner_copy(1).wait_recv()
    total = fin[...]
    for n in range(3):
        total = total + zd[n].astype(F32)
    total = total * (1.0 / 128.0)
    down_v[...] = total[:, :256]
    gate_v[...] = total[:, 256:512]
    up_v[...] = total[:, 512:]

    def left(ref, sem):
        pltpu.make_async_copy(ref, ref, sem).wait()

    with jax.named_scope("wait_sends"):
        left(s_send.at[:, pl.ds(0, 56)], ds_sem.at[0])
        left(sg_v.at[:, pl.ds(0, 56)], rs_sem.at[0])
        left(pgu.at[:, :, :, pl.ds(0, 56)], ws_sem.at[0, 0])
        left(pd.at[:, :, :, :, pl.ds(0, 896)], ws_sem.at[0, 1])
        left(drecv, cs_sem.at[0])
        left(lsend.at[is_far], cs_sem.at[1])
        left(ssend.at[is_far], cs_sem.at[5])
        left(lsend.at[1 - is_far, :, :, downs], cs_sem.at[2])
        left(ssend.at[1 - is_far, :, :, downs], cs_sem.at[6])
        left(lsend.at[pl.ds(2, 2)], cs_sem.at[3])
        left(ssend.at[pl.ds(2, 2)], cs_sem.at[7])
        left(finb.at[pl.ds(1, 2)], cs_sem.at[9])

        @pl.when(near)
        def _():
            left(pgu.at[0, pl.ds(0, 2)], ws_sem.at[1, 0])
            left(pd.at[0, pl.ds(0, 2)], ws_sem.at[1, 1])
            left(lsend.at[1, :, :, gates], cs_sem.at[4])
            left(ssend.at[1, :, :, gates], cs_sem.at[8])
            left(finb.at[0], cs_sem.at[10])

        @pl.when(far)
        def _():
            left(finb.at[0, :, downs], cs_sem.at[10])
            left(zsend, cs_sem.at[11])


def per_device(grad_out, routes, route_probs, dispatched, w_gate, w_up, w_down):
    wg = w_gate.reshape(2, 4, 2, 64, 256)
    wu = w_up.reshape(2, 4, 2, 64, 256)
    wd = w_down.reshape(2, 4, 2, 16, 1024)
    hbm = pl.BlockSpec(memory_space=pltpu.HBM)
    vmem = pl.BlockSpec(memory_space=pltpu.VMEM)
    dma = pltpu.SemaphoreType.DMA
    V = pltpu.VMEM
    results = pl.pallas_call(
        kernel,
        out_shape=(V((4, 64, 1024), BF16),) + (V((32, 256), F32),) * 3,
        in_specs=[hbm] * 7,
        out_specs=(vmem,) * 4,
        scratch_shapes=[
            V((4, 8, 64), jnp.int32),
            V((4, 8, 64), BF16),
            V((4, 64, 1024), BF16),
            V((4, 64, 1024), BF16),
            V((2, 4, 2, 64, 512), BF16),
            V((2, 4, 2, 16, 1024), BF16),
            V((2, 4, 2, 64, 512), BF16),
            V((2, 4, 2, 16, 1024), BF16),
            V((4, 64, 64), BF16),
            V((4, 64, 1024), BF16),
            V((4, 64, 1024), BF16),
            V((2, 2, 128, 256), F32),
            V((2, 2, 128, 256), F32),
            V((2, 128, 512), BF16),
            V((2, 2, 128, 512), BF16),
            V((4, 64, 1024), BF16),
            V((4, 64, 1024), BF16),
            V((2, 2, 8, 2, 32, 768), F32),
            V((2, 2, 8, 2, 32, 768), BF16),
            V((2, 2, 8, 32, 768), BF16),
            V((4, 4, 32, 768), BF16),
            V((4, 4, 32, 768), BF16),
            V((4, 3, 32, 768), BF16),
            V((4, 3, 32, 768), BF16),
            V((32, 768), F32),
            V((3, 32, 768), BF16),
            V((3, 32, 768), BF16),
            V((8, 32, 512), BF16),
            V((8, 32, 512), BF16),
            dma((6,)), dma((1,)),
            dma((1,)), dma((2,)), dma((1,)), dma((2,)),
            dma((2, 2)), dma((8, 2, 2)), dma((12,)), dma((2, 2)),
            dma((5, 4)), dma((5, 3)), dma((4,)),
        ],
        compiler_params=pltpu.CompilerParams(
            collective_id=0, has_side_effects=True, vmem_limit_bytes=48000000
        ),
        name="moe_backward",
    )(
        *(
            pltpu.with_memory_space_constraint(a, pltpu.HBM)
            for a in (
                grad_out, jnp.swapaxes(routes, 1, 2), jnp.swapaxes(route_probs, 1, 2), dispatched, wg, wu, wd
            )
        )
    )

    def store(a, b, c, d, out_a, out_b, out_c, out_d, sem):
        copies = [
            pltpu.make_async_copy(src, dst, sem.at[n])
            for n, (src, dst) in enumerate(((a, out_a), (b, out_b), (c, out_c), (d, out_d)))
        ]
        for copy in copies:
            copy.start()
        for copy in copies:
            copy.wait()

    return pl.pallas_call(
        store,
        out_shape=tuple(jax.ShapeDtypeStruct(r.shape, r.dtype) for r in results),
        in_specs=[vmem] * 4,
        out_specs=(hbm,) * 4,
        scratch_shapes=[dma((4,))],
        compiler_params=pltpu.CompilerParams(vmem_limit_bytes=1000000),
        name="store_results",
    )(*results)


def solution(mesh):
    return jax.shard_map(
        per_device,
        mesh=mesh,
        in_specs=(
            P(None, ("dp", "expert"), None),
            P(None, ("dp", "expert"), None),
            P(None, ("dp", "expert"), None),
            P(None, ("dp", "expert"), None),
            P(None, "expert"),
            P(None, "expert"),
            P("expert", None),
        ),
        out_specs=(
            P(None, ("dp", "expert"), None),
            P("dp", "expert"),
            P("dp", "expert"),
            P("dp", "expert"),
        ),
        check_vma=False,
    )
```

```python
import jax
import jax.numpy as jnp
from jax import lax
from jax.experimental import pallas as pl
from jax.experimental.pallas import tpu as pltpu
from jax.sharding import PartitionSpec as P

MESH = pl.DeviceIdType.MESH
F32 = jnp.float32
BF16 = jnp.bfloat16

NT = (((1,), (1,)), ((), ()))
TN = (((0,), (0,)), ((), ()))


def kernel(
    dy_hbm, routes_hbm, probs_hbm, disp_hbm, wg_hbm, wu_hbm, wd_hbm,
    gin_v, gate_v, up_v, down_v,
    routes_v, probs_v, dy_v, x_v, wgu, wd, pgu, pd,
    mix_v, s_send, s_recv, act_v, fac_v, hid_v, dg_v, sg_v, ret_v,
    rf, rb, drecv, lsend, lrecv, ssend, srecv, fin, finb, zd, zsend, zrecv,
    in_sem, x_sem,
    ds_sem, dr_sem, rs_sem, rr_sem,
    ws_sem, wr_sem, cs_sem, cr_sem,
    lsr_sem, ssr_sem, zr_sem,
):
    dp = lax.axis_index("dp")
    mem = lax.axis_index("expert")
    core = dp % 2
    y = (dp // 2) % 8
    zl = dp // 16
    step = 1 - 2 * core
    mine = mem // 2
    zh = mem % 4
    low = (zh * (3 - zh)) // 2

    def peer_of(e):
        return 4 * (e // 2) + low + (e % 2) * (3 - 2 * low)

    partner = mem + 1 - 2 * (mem % 2)
    dp_core = dp + 1 - 2 * core
    dp_fwd = zl * 16 + ((y + step + 8) % 8) * 2 + core
    dp_bwd = zl * 16 + ((y - step + 8) % 8) * 2 + core
    dp_z = (1 - zl) * 16 + y * 2 + core

    def remote(src, dst, ssem, rsem, dev):
        return pltpu.make_async_remote_copy(
            src_ref=src, dst_ref=dst, send_sem=ssem, recv_sem=rsem,
            device_id=dev, device_id_type=MESH,
        )

    barrier = pltpu.get_barrier_semaphore()
    peers = [(dp, peer_of((mine + i) % 8)) for i in range(1, 8)]
    peers += [(dp, partner), (dp_core, mem), (dp_fwd, mem), (dp_bwd, mem), (dp_z, mem), (dp_z, partner)]
    for dev in peers:
        pl.semaphore_signal(barrier, inc=1, device_id=dev, device_id_type=MESH)

    loads = [
        pltpu.make_async_copy(wg_hbm, wgu.at[:, :, :, :, pl.ds(0, 256)], in_sem.at[3]),
        pltpu.make_async_copy(wu_hbm, wgu.at[:, :, :, :, pl.ds(256, 256)], in_sem.at[4]),
        pltpu.make_async_copy(wd_hbm, wd, in_sem.at[5]),
        pltpu.make_async_copy(routes_hbm, routes_v, in_sem.at[0]),
        pltpu.make_async_copy(probs_hbm, probs_v, in_sem.at[1]),
        pltpu.make_async_copy(dy_hbm, dy_v, in_sem.at[2]),
    ]
    for load in loads:
        load.start()
    with jax.named_scope("barrier"):
        for load in loads[:3]:
            load.wait()
        pl.semaphore_wait(barrier, len(peers))

    quarter = y % 4

    def weights_copy(n, h, src_a, src_b, where, side, dev, come=None):
        come = n if come is None else come
        kind = 0 if 0 < n < 8 else 1
        return [
            remote(src_a.at[h, where, side], pgu.at[h, where, side], ws_sem.at[kind, 0], wr_sem.at[come, h, 0], dev),
            remote(src_b.at[h, where, side], pd.at[h, where, side], ws_sem.at[kind, 1], wr_sem.at[come, h, 1], dev),
        ]

    def start(copies):
        for copy in copies:
            copy.start()

    def weights_wait(n, h, where, side):
        for copy in weights_copy(n, h, pgu, pd, where, side, (dp_core, mem)):
            copy.wait_recv()

    def handle(n, h, where, onward):
        held = weights_copy(n, h, pgu, pd, where, core, (dp_core, mem))
        further = [weights_copy(to, h, pgu, pd, where, core, dev) for to, dev in onward]
        relay = weights_copy(8, h, pgu, pd, where, core, (dp_z, mem), 0) if n == 0 else ()
        for k in range(2):
            held[k].wait_recv()
            if n == 0:

                @pl.when(near)
                def _():
                    relay[k].start()

            for copies in further:
                copies[k].start()

    near = (zl + zh) % 2 == 1
    far = (zl + zh) % 2 == 0
    near_sends = []
    for h in range(2):
        near_sends += weights_copy(0, h, wgu, wd, quarter, core, (dp_z, partner))

    @pl.when(near)
    def _():
        for copy in near_sends:
            copy.start()

    with jax.named_scope("wait_in"):
        for load in loads[3:]:
            load.wait()

    def route(mb, carry):
        ids = routes_v[mb]
        probs = probs_v[mb].astype(F32)
        lane = lax.broadcasted_iota(jnp.int32, (64, 64), 1)
        row = lax.broadcasted_iota(jnp.int32, (64, 64), 0)
        expert = lax.shift_right_logical(row, 3)
        place = lax.bitwise_and(row, 7)
        hit = jnp.zeros((64, 64), F32)
        weight = jnp.zeros((64, 64), F32)
        for k in range(8):
            same = ids[k : k + 1, :] == expert
            hit = hit + jnp.where(same, 1.0, 0.0)
            weight = weight + jnp.where(same, probs[k : k + 1, :], 0.0)
        earlier = jnp.where(row < lane, 1.0, 0.0).astype(BF16)
        rank = jnp.dot(hit.astype(BF16), earlier, preferred_element_type=F32)
        chosen = jnp.where(rank == place.astype(F32), hit, 0.0)
        mix_v[mb] = chosen.astype(BF16)
        weighted = (chosen * weight).astype(BF16)
        scaled = jnp.dot(weighted, dy_v[mb], preferred_element_type=F32)
        s_send[mb] = scaled.astype(BF16)
        return carry

    x_loads = []
    for j in range(8):
        src = 4 * (j // 2) + (low if j % 2 == 0 else 3 - low)
        x_loads.append(
            pltpu.make_async_copy(
                disp_hbm.at[:, pl.ds(pl.multiple_of(src * 8, 8), 8)],
                x_v.at[:, pl.ds(j * 8, 8)],
                x_sem.at[0],
            )
        )
    for load in x_loads:
        load.start()
    def slots_copy(src, dst, sem_s, sem_r, chunk, i):
        to = (mine + i) % 8
        return remote(
            src.at[pl.ds(2 * chunk, 2), pl.ds(pl.multiple_of(to * 8, 8), 8)],
            dst.at[pl.ds(2 * chunk, 2), pl.ds(pl.multiple_of(mine * 8, 8), 8)],
            sem_s.at[0],
            sem_r.at[chunk],
            (dp, peer_of(to)),
        )

    def slots_self(src, dst, sem_r, chunk):
        at = pl.ds(pl.multiple_of(mine * 8, 8), 8)
        return pltpu.make_async_copy(
            src.at[pl.ds(2 * chunk, 2), at], dst.at[pl.ds(2 * chunk, 2), at], sem_r.at[chunk]
        )

    def slots_wait(dst, sem_r, chunk):
        rows = dst.at[pl.ds(2 * chunk, 2)]
        pltpu.make_async_copy(rows, rows, sem_r.at[chunk]).wait()

    crossing = []
    for chunk in range(2):
        with jax.named_scope("route"):
            lax.fori_loop(2 * chunk, 2 * chunk + 2, route, 0)
        start([slots_copy(s_send, s_recv, ds_sem, dr_sem, chunk, i) for i in (2, 4, 6)])
        slots_self(s_send, s_recv, dr_sem, chunk).start()
        across_z = [slots_copy(s_send, s_recv, ds_sem, dr_sem, chunk, i) for i in (1, 3, 5, 7)]
        crossing.extend(across_z)

        @pl.when(far)
        def _():
            for copy in across_z:
                copy.start()

    with jax.named_scope("wait_x"):
        pltpu.make_async_copy(x_v, x_v, x_sem.at[0]).wait()

    def hidden(half, weights):
        def body(chunk, carry):
            rows = x_v[pl.ds(2 * chunk, 2)].reshape(128, 1024)
            both = jnp.dot(rows, weights[...].reshape(1024, 512), preferred_element_type=F32)
            gate, up = both[:, :256], both[:, 256:]
            sig = jax.nn.sigmoid(gate)
            act = gate * sig
            act_v[half, chunk] = act
            fac_v[half, chunk] = up * sig * (1.0 + gate * (1.0 - sig))
            hid_v[chunk, :, pl.ds(256 * half, 256)] = (act * up).astype(BF16)
            return carry

        lax.fori_loop(0, 2, body, 0)

    def d_terms(half, chunk, down):
        rows = s_recv[pl.ds(2 * chunk, 2)].reshape(128, 1024)
        dh = lax.dot_general(rows, down[...].reshape(256, 1024), NT, preferred_element_type=F32)
        d_both = jnp.concatenate(
            [(dh * fac_v[half, chunk]).astype(BF16), (dh * act_v[half, chunk]).astype(BF16)], axis=1
        )
        dg_v[half, chunk] = d_both

    def slot_grads(chunk):
        total = lax.dot_general(
            dg_v[0, chunk], wgu[...].reshape(1024, 512), NT, preferred_element_type=F32
        ) + lax.dot_general(dg_v[1, chunk], pgu[...].reshape(1024, 512), NT, preferred_element_type=F32)
        sg_v[pl.ds(2 * chunk, 2)] = total.astype(BF16).reshape(2, 64, 1024)

    def weight_terms(half, s):
        z = (zl + 1 + s) % 2

        def body(q, carry):
            cols = pl.ds(pl.multiple_of((2 * z + q) * 256, 256), 256)
            at = pl.ds(4 * q, 4)
            right = hid_v[:, :, pl.ds(256 * half, 256)].reshape(256, 256)
            out = lax.dot_general(s_recv[:, :, cols].reshape(256, 256), right, TN, preferred_element_type=F32)
            out = out.reshape(4, 2, 32, 256)
            rf[half, s, at, :, :, pl.ds(0, 256)] = out
            rb[half, s, at, :, :, pl.ds(0, 256)] = out.astype(BF16)
            right = dg_v[half].reshape(256, 512)
            out = lax.dot_general(x_v[:, :, cols].reshape(256, 256), right, TN, preferred_element_type=F32)
            out = out.reshape(4, 2, 32, 512)
            rf[half, s, at, :, :, pl.ds(256, 512)] = out
            rb[half, s, at, :, :, pl.ds(256, 512)] = out.astype(BF16)
            return carry

        lax.fori_loop(0, 2, body, 0)
        start([core_copy(half, s)])

    is_far = (zl + zh + 1) % 2
    full = pl.ds(0, 768)
    downs = pl.ds(0, 256)
    gates = pl.ds(256, 512)
    streams = (
        (0, is_far, full),
        (0, 1 - is_far, downs),
        (1, 0, full),
        (1, 1, full),
        (0, 1, gates),
    )

    def core_copy(g, s):
        return remote(rb.at[g, s, :, 1 - core], drecv.at[g, s], cs_sem.at[0], cr_sem.at[g, s], (dp_core, mem))

    def term(n, owner):
        g, s, cols = streams[n]
        own = rf[g, s, owner, core, :, cols] + drecv[g, s, owner, :, cols].astype(F32)
        if n == 4:
            own = own + zrecv[owner].astype(F32)
        return own

    def at(ref, n, t):
        g, s, cols = streams[n]
        return ref.at[2 * g + s, t, :, cols]

    group = (1, 2, 3, 3, 4)

    def long_copy(n, t):
        return remote(at(lsend, n, t), at(lrecv, n, t), cs_sem.at[group[n]], lsr_sem.at[n, t], (dp_fwd, mem))

    def short_copy(n, t):
        return remote(at(ssend, n, t), at(srecv, n, t), cs_sem.at[group[n] + 4], ssr_sem.at[n, t], (dp_bwd, mem))

    def ring_first(n):
        at(lsend, n, 0)[...] = term(n, (y + 4) % 8).astype(BF16)
        start([long_copy(n, 0)])
        at(ssend, n, 0)[...] = term(n, (y - 3 * step + 8) % 8).astype(BF16)
        start([short_copy(n, 0)])

    def ring_next(n, t):
        own = term(n, (y + (4 - t) * step + 8) % 8)
        long_copy(n, t - 1).wait_recv()
        at(lsend, n, t)[...] = (own + at(lrecv, n, t - 1)[...].astype(F32)).astype(BF16)
        start([long_copy(n, t)])
        if t < 3:
            own = term(n, (y - (3 - t) * step + 8) % 8)
            short_copy(n, t - 1).wait_recv()
            at(ssend, n, t)[...] = (own + at(srecv, n, t - 1)[...].astype(F32)).astype(BF16)
            start([short_copy(n, t)])

    def ring_total(n):
        own = term(n, y)
        short_copy(n, 2).wait_recv()
        own = own + at(srecv, n, 2)[...].astype(F32)
        long_copy(n, 3).wait_recv()
        return own + at(lrecv, n, 3)[...].astype(F32)

    def partner_copy(s):
        return remote(finb.at[1 + s], zd.at[1 + s], cs_sem.at[9], zr_sem.at[1 + s], ((dp_z, dp)[s], partner))

    def other_z_copy(cols):
        return remote(finb.at[0, :, cols], zd.at[0, :, cols], cs_sem.at[10], zr_sem.at[0], (dp_z, mem))

    def z_first():
        return remote(zsend, zrecv, cs_sem.at[11], zr_sem.at[3], (dp_z, mem))

    def ring_last(n):
        if n in (2, 3):
            finb[n - 1] = ring_total(n).astype(BF16)
            start([partner_copy(n - 2)])
        elif n == 4:
            fin[:, gates] = ring_total(n)
        else:
            own = ring_total(n)
            cols = streams[n][2]
            sends_on, keeps = (near, far) if n == 0 else (far, near)

            @pl.when(sends_on)
            def _():
                finb[0, :, cols] = own.astype(BF16)
                other_z_copy(cols).start()

            @pl.when(keeps)
            def _():
                fin[:, cols] = own

    def slots_arrive(chunk):
        slots_wait(s_recv, dr_sem, chunk)

    from_bwd = (y - step + 8) % 4
    from_fwd = (y + step + 8) % 4
    across = (y + 2) % 4

    def first_piece(h):
        handle(0, h, quarter, ((1, (dp_fwd, mem)), (2, (dp_bwd, mem)), (4, (dp_core, mem))))

    def second_piece(h):
        handle(1, h, from_bwd, ((3, (dp_fwd, mem)), (5, (dp_core, mem))))
        handle(2, h, from_fwd, ((6, (dp_core, mem)),))

    def third_piece(h):
        handle(3, h, across, ((7, (dp_core, mem)),))

    def last_piece(h):
        weights_wait(4, h, quarter, 1 - core)
        weights_wait(5, h, from_fwd, 1 - core)
        weights_wait(6, h, from_bwd, 1 - core)
        weights_wait(7, h, across, 1 - core)

    def tokens(chunk):
        slots_wait(ret_v, rr_sem, chunk)
        for mb in (2 * chunk, 2 * chunk + 1):
            gin_v[mb] = lax.dot_general(mix_v[mb], ret_v[mb], TN, preferred_element_type=F32).astype(BF16)

    with jax.named_scope("hidden0"):
        hidden(0, wgu)
    with jax.named_scope("w0a"):
        first_piece(0)
    with jax.named_scope("w0b"):
        first_piece(1)

    @pl.when(near)
    def _():
        for copy in crossing:
            copy.start()

    with jax.named_scope("w1a"):
        second_piece(0)
    with jax.named_scope("w1b"):
        second_piece(1)
    with jax.named_scope("slots0"):
        slots_arrive(0)
    with jax.named_scope("d_own0"):
        d_terms(0, 0, wd)
    with jax.named_scope("slots1"):
        slots_arrive(1)
    with jax.named_scope("d_own1"):
        d_terms(0, 1, wd)
    with jax.named_scope("weights0"):
        weight_terms(0, 0)
        weight_terms(0, 1)
    with jax.named_scope("w3"):
        third_piece(0)
        third_piece(1)
    with jax.named_scope("wlast"):
        last_piece(0)
        last_piece(1)
    with jax.named_scope("hidden1"):
        hidden(1, pgu)
    with jax.named_scope("ring_first0"):
        core_copy(0, 0).wait_recv()
        core_copy(0, 1).wait_recv()
        ring_first(0)

    @pl.when(far)
    def _():
        zsend[...] = (rf[0, 0, :, core, :, gates] + drecv[0, 0, :, :, gates].astype(F32)).astype(BF16)
        z_first().start()

    with jax.named_scope("ring_first0b"):
        ring_first(1)
    with jax.named_scope("d_partner"):
        d_terms(1, 0, pd)
        d_terms(1, 1, pd)
    with jax.named_scope("weights1"):
        weight_terms(1, 0)
        weight_terms(1, 1)
    with jax.named_scope("ring_next0_1"):
        ring_next(0, 1)
        ring_next(1, 1)
    with jax.named_scope("ring_first1"):
        for s in range(2):
            core_copy(1, s).wait_recv()
            ring_first(2 + s)
    with jax.named_scope("slot_grads0"):
        slot_grads(0)
        start([slots_copy(sg_v, ret_v, rs_sem, rr_sem, 0, i) for i in range(1, 8)])
        slots_self(sg_v, ret_v, rr_sem, 0).start()
    with jax.named_scope("ring_next0_2"):
        ring_next(0, 2)
        ring_next(1, 2)
    with jax.named_scope("slot_grads1"):
        slot_grads(1)
        start([slots_copy(sg_v, ret_v, rs_sem, rr_sem, 1, i) for i in range(1, 8)])
        slots_self(sg_v, ret_v, rr_sem, 1).start()
    with jax.named_scope("ring_next1_1"):
        ring_next(2, 1)
        ring_next(3, 1)
    with jax.named_scope("ring_next0_3"):
        ring_next(0, 3)
        ring_next(1, 3)
    with jax.named_scope("ring_next1_2"):
        ring_next(2, 2)
        ring_next(3, 2)
    with jax.named_scope("ring_last0"):
        ring_last(0)
        ring_last(1)

    @pl.when(near)
    def _():
        z_first().wait_recv()
        ring_first(4)

    with jax.named_scope("ring_next1_3"):
        ring_next(2, 3)
        ring_next(3, 3)

    @pl.when(near)
    def _():
        ring_next(4, 1)

    with jax.named_scope("ring_last1"):
        ring_last(2)
        ring_last(3)
    with jax.named_scope("tokens0"):
        tokens(0)

    @pl.when(near)
    def _():
        ring_next(4, 2)


    with jax.named_scope("late"):

        @pl.when(near)
        def _():
            ring_next(4, 3)
            ring_last(4)
            zd[0, :, gates] = jnp.zeros((32, 512), BF16)
            other_z_copy(downs).wait_recv()

        @pl.when(far)
        def _():
            other_z_copy(full).wait_recv()

    with jax.named_scope("tokens1"):
        tokens(1)
    with jax.named_scope("wait_z"):
        partner_copy(0).wait_recv()
        partner_copy(1).wait_recv()
    total = fin[...]
    for n in range(3):
        total = total + zd[n].astype(F32)
    total = total * (1.0 / 128.0)
    down_v[...] = total[:, :256]
    gate_v[...] = total[:, 256:512]
    up_v[...] = total[:, 512:]

    def left(ref, sem):
        pltpu.make_async_copy(ref, ref, sem).wait()

    with jax.named_scope("wait_sends"):
        left(s_send.at[:, pl.ds(0, 56)], ds_sem.at[0])
        left(sg_v.at[:, pl.ds(0, 56)], rs_sem.at[0])
        left(pgu.at[:, :, :, pl.ds(0, 56)], ws_sem.at[0, 0])
        left(pd.at[:, :, :, :, pl.ds(0, 896)], ws_sem.at[0, 1])
        left(drecv, cs_sem.at[0])
        left(lsend.at[is_far], cs_sem.at[1])
        left(ssend.at[is_far], cs_sem.at[5])
        left(lsend.at[1 - is_far, :, :, downs], cs_sem.at[2])
        left(ssend.at[1 - is_far, :, :, downs], cs_sem.at[6])
        left(lsend.at[pl.ds(2, 2)], cs_sem.at[3])
        left(ssend.at[pl.ds(2, 2)], cs_sem.at[7])
        left(finb.at[pl.ds(1, 2)], cs_sem.at[9])

        @pl.when(near)
        def _():
            left(pgu.at[0, pl.ds(0, 2)], ws_sem.at[1, 0])
            left(pd.at[0, pl.ds(0, 2)], ws_sem.at[1, 1])
            left(lsend.at[1, :, :, gates], cs_sem.at[4])
            left(ssend.at[1, :, :, gates], cs_sem.at[8])
            left(finb.at[0], cs_sem.at[10])

        @pl.when(far)
        def _():
            left(finb.at[0, :, downs], cs_sem.at[10])
            left(zsend, cs_sem.at[11])


def per_device(grad_out, routes, route_probs, dispatched, w_gate, w_up, w_down):
    wg = w_gate.reshape(2, 4, 2, 64, 256)
    wu = w_up.reshape(2, 4, 2, 64, 256)
    wd = w_down.reshape(2, 4, 2, 16, 1024)
    hbm = pl.BlockSpec(memory_space=pltpu.HBM)
    vmem = pl.BlockSpec(memory_space=pltpu.VMEM)
    dma = pltpu.SemaphoreType.DMA
    V = pltpu.VMEM
    results = pl.pallas_call(
        kernel,
        out_shape=(V((4, 64, 1024), BF16),) + (V((32, 256), F32),) * 3,
        in_specs=[hbm] * 7,
        out_specs=(vmem,) * 4,
        scratch_shapes=[
            V((4, 8, 64), jnp.int32),
            V((4, 8, 64), BF16),
            V((4, 64, 1024), BF16),
            V((4, 64, 1024), BF16),
            V((2, 4, 2, 64, 512), BF16),
            V((2, 4, 2, 16, 1024), BF16),
            V((2, 4, 2, 64, 512), BF16),
            V((2, 4, 2, 16, 1024), BF16),
            V((4, 64, 64), BF16),
            V((4, 64, 1024), BF16),
            V((4, 64, 1024), BF16),
            V((2, 2, 128, 256), F32),
            V((2, 2, 128, 256), F32),
            V((2, 128, 512), BF16),
            V((2, 2, 128, 512), BF16),
            V((4, 64, 1024), BF16),
            V((4, 64, 1024), BF16),
            V((2, 2, 8, 2, 32, 768), F32),
            V((2, 2, 8, 2, 32, 768), BF16),
            V((2, 2, 8, 32, 768), BF16),
            V((4, 4, 32, 768), BF16),
            V((4, 4, 32, 768), BF16),
            V((4, 3, 32, 768), BF16),
            V((4, 3, 32, 768), BF16),
            V((32, 768), F32),
            V((3, 32, 768), BF16),
            V((3, 32, 768), BF16),
            V((8, 32, 512), BF16),
            V((8, 32, 512), BF16),
            dma((6,)), dma((1,)),
            dma((1,)), dma((2,)), dma((1,)), dma((2,)),
            dma((2, 2)), dma((8, 2, 2)), dma((12,)), dma((2, 2)),
            dma((5, 4)), dma((5, 3)), dma((4,)),
        ],
        compiler_params=pltpu.CompilerParams(
            collective_id=0, has_side_effects=True, vmem_limit_bytes=48000000
        ),
        name="moe_backward",
    )(
        *(
            pltpu.with_memory_space_constraint(a, pltpu.HBM)
            for a in (
                grad_out, jnp.swapaxes(routes, 1, 2), jnp.swapaxes(route_probs, 1, 2), dispatched, wg, wu, wd
            )
        )
    )

    def store(a, b, c, d, out_a, out_b, out_c, out_d, sem):
        copies = [
            pltpu.make_async_copy(src, dst, sem.at[n])
            for n, (src, dst) in enumerate(((a, out_a), (b, out_b), (c, out_c), (d, out_d)))
        ]
        for copy in copies:
            copy.start()
        for copy in copies:
            copy.wait()

    return pl.pallas_call(
        store,
        out_shape=tuple(jax.ShapeDtypeStruct(r.shape, r.dtype) for r in results),
        in_specs=[vmem] * 4,
        out_specs=(hbm,) * 4,
        scratch_shapes=[dma((4,))],
        compiler_params=pltpu.CompilerParams(vmem_limit_bytes=1000000),
        name="store_results",
    )(*results)


def solution(mesh):
    return jax.shard_map(
        per_device,
        mesh=mesh,
        in_specs=(
            P(None, ("dp", "expert"), None),
            P(None, ("dp", "expert"), None),
            P(None, ("dp", "expert"), None),
            P(None, ("dp", "expert"), None),
            P(None, "expert"),
            P(None, "expert"),
            P("expert", None),
        ),
        out_specs=(
            P(None, ("dp", "expert"), None),
            P("dp", "expert"),
            P("dp", "expert"),
            P("dp", "expert"),
        ),
        check_vma=False,
    )
```
